32 devices in a mesh: dp: 8 (over z, x), mp: 4 (over y, core).
Axes of the slice: x: 2, y: 2, z: 4, core: 2. Of those that a mesh axis runs over, the one named last changes fastest.
Arguments:
- query_rows: bfloat16 [2048, 2048], P('dp', 'mp'), may hold values from -6 to 6
- key_rows: bfloat16 [2048, 512], P('dp', 'mp'), may hold values from -6 to 6
- value_matrix: bfloat16 [2048, 512], P('dp', 'mp'), may hold values from -6 to 6
- out_weight: bfloat16 [2048, 5120], P('mp', 'dp'), may hold values from -0.125 to 0.125
- out_grad: bfloat16 [2048, 5120], P('dp', 'mp'), may hold values from -6 to 6
- doc_lengths: int32 [8, 8], P('dp'), may hold values from 1 to 249, as said below
Outputs:
- layer_out: bfloat16 [2048, 5120], P('dp', 'mp')
- query_grad: bfloat16 [2048, 2048], P('dp', 'mp')
- key_grad: bfloat16 [2048, 512], P('dp', 'mp')
- value_grad: bfloat16 [2048, 512], P('dp', 'mp')
- weight_grad: float32 [2048, 5120], P('mp', 'dp')
The draws below stay inside these ranges and needn't reach their ends.
Inputs may be any that keep to these rules, and one draw needn't show every extreme that they name: `doc_lengths`: each row holds 8 lengths of 1 or more that sum to 256.
All inputs are finite; a program needn't handle non-finite values.
Results may differ from the reference program's by a relative error of at most 0.014.
Values may be sent and summed in bfloat16 or wider, within the bound.
A program may use at most 64 MiB of HBM per device.

```python
import jax
import jax.numpy as jnp
from jax import lax

D = 5120
HQ = 16
KEY_VALUE_HEADS = 4
HEAD_WIDTH = 128
SEQ_DEV = 8
TOK_DEV = 256
TOKEN_TOTAL = 2048
N_DP = 8
N_MP = 4


def drawn_pair(key):
    base = jax.random.fold_in(key, 4021)
    query_key, key_random_seed = jax.random.split(base, 2)
    queries = jax.random.truncated_normal(query_key, -6.0, 6.0, (TOKEN_TOTAL, HQ * HEAD_WIDTH), jnp.float32)
    sampled_keys = jax.random.truncated_normal(key_random_seed, -6.0, 6.0, (TOKEN_TOTAL, KEY_VALUE_HEADS * HEAD_WIDTH), jnp.float32)
    return (queries, sampled_keys)


def draw_query_rows(key, part):
    return drawn_pair(key)[0].astype(jnp.bfloat16)


def draw_key_rows(key, part):
    return drawn_pair(key)[1].astype(jnp.bfloat16)


def draw_doc_lengths(key, part):
    base = jax.random.fold_in(key, 977)
    random_key, shift_key = jax.random.split(base)
    positions = jnp.arange(1, TOK_DEV, dtype=jnp.int32)
    shifts = jax.random.randint(shift_key, (N_DP, 1), 0, TOK_DEV, dtype=jnp.int32)
    device_rows = jnp.arange(N_DP, dtype=jnp.int32)[:, None]
    shifts = jnp.where(device_rows == 0, TOK_DEV - SEQ_DEV + 1, shifts)
    random_part = jax.random.randint(random_key, (N_DP, TOK_DEV - 1), 0, 4096, dtype=jnp.int32)
    scores = (random_part + 4096 * (positions[None, :] >= shifts).astype(jnp.int32)) * TOK_DEV + positions[None, :]
    picked = lax.top_k(scores, SEQ_DEV - 1)[1].astype(jnp.int32)
    cut_points = jnp.sort(picked + 1, axis=1)
    bounds = jnp.concatenate([jnp.zeros((N_DP, 1), jnp.int32), cut_points, jnp.full((N_DP, 1), TOK_DEV, jnp.int32)], axis=1)
    return jnp.diff(bounds, axis=1).astype(jnp.int32)


def raised(array, stream_key, source, target, parts, factor):
    def block_of(dim):
        return (jnp.arange(array.shape[dim]) // (array.shape[dim] // parts)).reshape((-1,) + (1,) * (array.ndim - 1 - dim))

    one_side = jax.random.permutation(stream_key, parts)[block_of(target)]
    other_side = (block_of(target) + parts // 2) % parts
    return jnp.where((block_of(source) == one_side) | (block_of(source) == other_side), factor * array, array)


def shard_levels(rng, extent, cuts, least, largest):
    gain = 1.0
    for axis_at, blocks in cuts:
        steps = jax.random.uniform(jax.random.fold_in(jax.random.fold_in(rng, 6), axis_at), (blocks,), jnp.float32, least / len(cuts), largest / len(cuts))
        gain = gain * jnp.repeat(jnp.exp(steps), extent[axis_at] // blocks).reshape((-1,) + (1,) * (len(extent) - 1 - axis_at))
    return gain


def normal_values(key, dims, spread, reach, shards=(), kind=jnp.bfloat16):
    drawn = spread * jax.random.normal(key, dims, jnp.float32)
    if shards:
        drawn = drawn * shard_levels(key, dims, shards, -0.22, 0.18)
    return jnp.clip(drawn, -reach, reach).astype(kind)


def gaussian_with(stream_key, extent, deviation, bound, cuts, heavy, kind=jnp.bfloat16):
    entries = deviation * jax.random.normal(stream_key, extent, jnp.float32)
    if cuts:
        entries = entries * shard_levels(stream_key, extent, cuts, -0.22, 0.18)
    return jnp.clip(raised(entries, jax.random.fold_in(stream_key, 3), *heavy), -bound, bound).astype(kind)


def setup_inputs(seed: int = 0) -> dict:
    streams_of = jax.random.split(jax.random.key(seed), 7)
    return {
        "query_rows": draw_query_rows(jax.random.fold_in(streams_of[6], 71), 0),
        "key_rows": draw_key_rows(jax.random.fold_in(streams_of[6], 71), 0),
        "value_matrix": normal_values(streams_of[2], (TOKEN_TOTAL, KEY_VALUE_HEADS * HEAD_WIDTH), 1.0, 6.0, ((0, 8), (1, 4))),
        "out_weight": normal_values(streams_of[3], (HQ * HEAD_WIDTH, D), (HQ * HEAD_WIDTH) ** -0.5, 0.125, ((0, 4), (1, 8))),
        "out_grad": gaussian_with(streams_of[4], (TOKEN_TOTAL, D), 1.0, 6.0, ((0, 8), (1, 4)), (0, 1, 8, 2.0)),
        "doc_lengths": draw_doc_lengths(jax.random.fold_in(streams_of[6], 71), 0),
    }


def local_segments(lengths, row_count):
    segment_ends = jnp.cumsum(lengths)
    positions = jnp.arange(row_count, dtype=jnp.int32)
    return jnp.sum((positions[:, None] >= segment_ends[None, :]).astype(jnp.int32), axis=1)


def split_heads(matrix):
    row_count = matrix.shape[0]
    return matrix.astype(jnp.float32).reshape(row_count, matrix.shape[1] // HEAD_WIDTH, HEAD_WIDTH).transpose(1, 0, 2)


def join_heads(tensor):
    return tensor.transpose(1, 0, 2).reshape(tensor.shape[1], tensor.shape[0] * HEAD_WIDTH)


def device_attention(queries_in, keys_in, values_in, upstream, segment):
    row_count = queries_in.shape[0]
    queries = split_heads(queries_in)
    kv_count = keys_in.shape[1] // HEAD_WIDTH
    group_size = queries.shape[0] // kv_count
    key_heads = jnp.repeat(split_heads(keys_in), group_size, axis=0)
    value_heads = jnp.repeat(split_heads(values_in), group_size, axis=0)
    upstreams = split_heads(upstream)
    softmax_scale = HEAD_WIDTH ** -0.5
    positions = jnp.arange(row_count, dtype=jnp.int32)
    allowed = (segment[:, None] == segment[None, :]) & (positions[:, None] >= positions[None, :])
    logits = jnp.einsum("hid,hjd->hij", queries, key_heads) * softmax_scale
    logits = jnp.where(allowed[None], logits, -jnp.inf)
    row_max = jnp.max(logits, axis=-1, keepdims=True)
    exp_terms = jnp.exp(logits - row_max)
    probability = exp_terms / jnp.sum(exp_terms, axis=-1, keepdims=True)
    weights = probability.astype(jnp.bfloat16).astype(jnp.float32)
    attended = jnp.einsum("hij,hjd->hid", weights, value_heads).astype(jnp.bfloat16)
    prob_grad = jnp.einsum("hid,hjd->hij", upstreams, value_heads)
    row_delta = jnp.sum(probability * prob_grad, axis=-1, keepdims=True)
    score_grad = (probability * (prob_grad - row_delta) * softmax_scale).astype(jnp.bfloat16).astype(jnp.float32)
    query_grad = jnp.einsum("hij,hjd->hid", score_grad, key_heads).astype(jnp.bfloat16)
    key_full = jnp.einsum("hij,hid->hjd", score_grad, queries)
    value_full = jnp.einsum("hij,hid->hjd", weights, upstreams)
    key_grad = key_full.reshape(kv_count, group_size, row_count, HEAD_WIDTH).sum(axis=1).astype(jnp.bfloat16)
    value_grad = value_full.reshape(kv_count, group_size, row_count, HEAD_WIDTH).sum(axis=1).astype(jnp.bfloat16)
    return join_heads(attended), join_heads(query_grad), join_heads(key_grad), join_heads(value_grad)


def reference(query_rows, key_rows, value_matrix, out_weight, out_grad, doc_lengths):
    attn_grad = jnp.dot(out_grad, out_weight.T, preferred_element_type=jnp.float32).astype(jnp.bfloat16)

    def per_device(pieces):
        queries_in, keys_in, values_in, upstream, lengths = pieces
        segment = local_segments(lengths, TOK_DEV)
        return device_attention(queries_in, keys_in, values_in, upstream, segment)

    stacked = (query_rows.reshape(N_DP, TOK_DEV, -1), key_rows.reshape(N_DP, TOK_DEV, -1),
               value_matrix.reshape(N_DP, TOK_DEV, -1), attn_grad.reshape(N_DP, TOK_DEV, -1), doc_lengths)
    attended, query_grad, key_grad, value_grad = lax.map(per_device, stacked)
    attended = attended.reshape(TOKEN_TOTAL, -1)
    query_grad = query_grad.reshape(TOKEN_TOTAL, -1)
    key_grad = key_grad.reshape(TOKEN_TOTAL, -1)
    value_grad = value_grad.reshape(TOKEN_TOTAL, -1)
    group_width = HQ * HEAD_WIDTH // N_MP
    total = jnp.zeros((TOKEN_TOTAL, D), jnp.float32)
    for group_index in range(N_MP):
        low_edge = group_index * group_width
        partial_sum = jnp.dot(attended[:, low_edge:low_edge + group_width], out_weight[low_edge:low_edge + group_width],
                              preferred_element_type=jnp.float32).astype(jnp.bfloat16)
        total = total + lax.optimization_barrier(partial_sum).astype(jnp.float32)
    layer_out = total.astype(jnp.bfloat16)
    weight_grad = jnp.dot(attended.T, out_grad, preferred_element_type=jnp.float32)
    return (layer_out, query_grad, key_grad, value_grad, weight_grad)
```

```python
import functools

import jax
import jax.numpy as jnp
from jax import lax
from jax.experimental import pallas as pl
from jax.experimental.pallas import tpu as pltpu
from jax.sharding import PartitionSpec as P

HEAD_WIDTH = 128
TILE = 128


def local_segments(lengths, row_count):
    segment_ends = jnp.cumsum(lengths)
    positions = jnp.arange(row_count, dtype=jnp.int32)
    return jnp.sum((positions[:, None] >= segment_ends[None, :]).astype(jnp.int32), axis=1)


def to_heads(matrix):
    return matrix.reshape(matrix.shape[0], matrix.shape[1] // HEAD_WIDTH, HEAD_WIDTH).transpose(
        1, 0, 2
    )


def from_heads(tensor):
    return tensor.transpose(1, 0, 2).reshape(tensor.shape[1], tensor.shape[0] * tensor.shape[2])


def attend(queries, key_rows, value_matrix, upstreams, segment):
    head_count, row_count, head_size = queries.shape
    tile_rows = min(TILE, row_count)
    block_count = row_count // tile_rows
    softmax_scale = HEAD_WIDTH ** (-0.5)
    offsets = jnp.arange(tile_rows, dtype=jnp.int32)
    empty_rows = jnp.zeros((tile_rows, head_size), jnp.float32)
    key_sums = [empty_rows] * block_count
    value_sums = [empty_rows] * block_count
    attended_blocks = []
    grad_blocks = []
    for block_index in range(block_count):
        row_start = block_index * tile_rows
        query_tile = queries[:, row_start : row_start + tile_rows]
        upstream_tile = upstreams[:, row_start : row_start + tile_rows]
        query_segment = segment[row_start : row_start + tile_rows]
        active = [
            segment[(column_index + 1) * tile_rows - 1] >= query_segment[0]
            for column_index in range(block_index + 1)
        ]
        score_tiles = []
        for column_index in range(block_index + 1):
            column_start = column_index * tile_rows
            key_tile = key_rows[column_start : column_start + tile_rows]
            key_segment = segment[column_start : column_start + tile_rows]
            allowed = (query_segment[:, None] == key_segment[None, :]) & (
                (row_start + offsets)[:, None] >= (column_start + offsets)[None, :]
            )

            def score_tile(query_tile=query_tile, key_tile=key_tile, allowed=allowed):
                logits = (
                    jnp.einsum(
                        "hid,jd->hij", query_tile, key_tile, preferred_element_type=jnp.float32
                    )
                    * softmax_scale
                )
                return jnp.where(allowed[None], logits, -jnp.inf)

            def masked_tile():
                return jnp.full((head_count, tile_rows, tile_rows), -jnp.inf, jnp.float32)

            score_tiles.append(lax.cond(active[column_index], score_tile, masked_tile))
        logits = jnp.concatenate(score_tiles, axis=-1)
        row_max = jnp.max(logits, axis=-1, keepdims=True)
        exp_terms = jnp.exp(logits - row_max)
        probability = exp_terms / jnp.sum(exp_terms, axis=-1, keepdims=True)
        weights = probability.astype(jnp.bfloat16)
        attended = jnp.zeros((head_count, tile_rows, head_size), jnp.float32)
        grad_tiles = []
        for column_index in range(block_index + 1):
            column_start = column_index * tile_rows
            value_tile = value_matrix[column_start : column_start + tile_rows]
            weight_tile = weights[:, :, column_start : column_start + tile_rows]

            def forward_tile(
                weight_tile=weight_tile, value_tile=value_tile, upstream_tile=upstream_tile
            ):
                return (
                    jnp.einsum(
                        "hij,jd->hid", weight_tile, value_tile, preferred_element_type=jnp.float32
                    ),
                    jnp.einsum(
                        "hid,jd->hij", upstream_tile, value_tile, preferred_element_type=jnp.float32
                    ),
                )

            def empty_pair():
                return (
                    jnp.zeros((head_count, tile_rows, head_size), jnp.float32),
                    jnp.zeros((head_count, tile_rows, tile_rows), jnp.float32),
                )

            contribution, prob_grad_tile = lax.cond(active[column_index], forward_tile, empty_pair)
            attended = attended + contribution
            grad_tiles.append(prob_grad_tile)
        prob_grad = jnp.concatenate(grad_tiles, axis=-1)
        row_delta = jnp.sum(probability * prob_grad, axis=-1, keepdims=True)
        score_grad = (probability * (prob_grad - row_delta) * softmax_scale).astype(jnp.bfloat16)
        query_sum = jnp.zeros((head_count, tile_rows, head_size), jnp.float32)
        for column_index in range(block_index + 1):
            column_start = column_index * tile_rows
            key_tile = key_rows[column_start : column_start + tile_rows]
            score_piece = score_grad[:, :, column_start : column_start + tile_rows]
            weight_tile = weights[:, :, column_start : column_start + tile_rows]

            def backward_tile(
                score_piece=score_piece,
                key_tile=key_tile,
                weight_tile=weight_tile,
                query_tile=query_tile,
                upstream_tile=upstream_tile,
            ):
                return (
                    jnp.einsum(
                        "hij,jd->hid", score_piece, key_tile, preferred_element_type=jnp.float32
                    ),
                    jnp.einsum(
                        "hij,hid->jd", score_piece, query_tile, preferred_element_type=jnp.float32
                    ),
                    jnp.einsum(
                        "hij,hid->jd",
                        weight_tile,
                        upstream_tile,
                        preferred_element_type=jnp.float32,
                    ),
                )

            def empty_triple():
                return (
                    jnp.zeros((head_count, tile_rows, head_size), jnp.float32),
                    empty_rows,
                    empty_rows,
                )

            query_part, key_part, value_part = lax.cond(
                active[column_index], backward_tile, empty_triple
            )
            query_sum = query_sum + query_part
            key_sums[column_index] = key_sums[column_index] + key_part
            value_sums[column_index] = value_sums[column_index] + value_part
        attended_blocks.append(attended.astype(jnp.bfloat16))
        grad_blocks.append(query_sum.astype(jnp.bfloat16))
    return (
        jnp.concatenate(attended_blocks, axis=1),
        jnp.concatenate(grad_blocks, axis=1),
        jnp.concatenate(key_sums, axis=0),
        jnp.concatenate(value_sums, axis=0),
    )


def grad_term(grad_full, attended_heads):
    attended_flat = from_heads(attended_heads)
    return lax.dot_general(
        grad_full, attended_flat, (((0,), (0,)), ((), ())), preferred_element_type=jnp.float32
    )


def per_device(query_rows, key_rows, value_matrix, out_weight, out_grad, doc_lengths):
    row_count = query_rows.shape[0]
    weight_full = lax.all_gather(out_weight, "dp", axis=1, tiled=True)
    grad_full = lax.all_gather(out_grad, "mp", axis=1, tiled=True)
    attn_grad = lax.dot_general(
        grad_full, weight_full, (((1,), (1,)), ((), ())), preferred_element_type=jnp.float32
    ).astype(jnp.bfloat16)
    segment = local_segments(doc_lengths[0], row_count)
    queries = to_heads(query_rows)
    upstreams = to_heads(attn_grad)
    attended, query_grad, key_sum, value_sum = attend(
        queries, key_rows, value_matrix, upstreams, segment
    )
    key_grad = key_sum.astype(jnp.bfloat16)
    value_grad = value_sum.astype(jnp.bfloat16)
    weight_part = lax.psum_scatter(
        grad_term(grad_full, attended), "dp", scatter_dimension=0, tiled=True
    )
    attended_flat = from_heads(attended)
    query_grad = from_heads(query_grad)
    partial_sum = jnp.dot(attended_flat, weight_full, preferred_element_type=jnp.float32).astype(
        jnp.bfloat16
    )
    layer_out = lax.psum_scatter(
        lax.optimization_barrier(partial_sum).astype(jnp.float32).astype(jnp.bfloat16),
        "mp",
        scatter_dimension=1,
        tiled=True,
    )
    return (layer_out, query_grad, key_grad, value_grad, weight_part.T)


def dot(a, b, dims):
    return lax.dot_general(a, b, (dims, ((), ())), preferred_element_type=jnp.float32)


NN = ((1,), (0,))
NT = ((1,), (1,))
TN = ((0,), (0,))


def allowed_pairs(lengths_ref, rows):
    row_at = lax.broadcasted_iota(jnp.int32, (rows, 1), 0)
    column_at = lax.broadcasted_iota(jnp.int32, (1, rows), 1)
    row_segment = jnp.zeros((rows, 1), jnp.int32)
    column_segment = jnp.zeros((1, rows), jnp.int32)
    end = jnp.int32(0)
    for index in range(lengths_ref.shape[1]):
        end = end + lengths_ref[0, index]
        row_segment = row_segment + jnp.where(row_at >= end, 1, 0)
        column_segment = column_segment + jnp.where(column_at >= end, 1, 0)
    return (row_segment == column_segment) & (row_at >= column_at)


def branch_kernel(
    n_dp,
    n_mp,
    lengths_ref,
    query_ref,
    key_ref,
    value_ref,
    weight_ref,
    grad_ref,
    layer_ref,
    query_grad_ref,
    key_grad_ref,
    value_grad_ref,
    weight_grad_ref,
    weight_all,
    grads,
    relay_in,
    heads_all,
    heads_turned,
    up_own,
    up_in,
    up_out,
    layer_part,
    pair_in,
    pair_out,
    tier_in,
    layer_sum,
    layer_in,
    twin_out,
    twin_in,
    probs,
    weight_send,
    weight_recv,
    swap_send,
    relay_send,
    relay_recv,
    grad_recv,
    lift_send,
    side_send,
    side_recv,
    heads_send,
    heads_recv,
    up_send,
    up_recv,
    pair_send,
    pair_recv,
    tier_send,
    tier_recv,
    done_send,
    done_recv,
    twin_send,
    twin_recv,
):
    d = lax.axis_index("dp")
    m = lax.axis_index("mp")
    line = n_dp // 2
    tiers = n_mp // 2
    rows = query_ref.shape[0]
    part = rows // n_mp
    width = query_ref.shape[1]
    columns = weight_ref.shape[1]
    span = grad_ref.shape[1]
    head_count = width // HEAD_WIDTH
    group_size = width // key_ref.shape[1]
    scale = HEAD_WIDTH ** (-0.5)
    spot = lax.div(d, 2)
    side = lax.rem(d, 2)
    twin = d + 1 - 2 * side
    core = lax.rem(m, 2)
    tier = lax.div(m, 2)
    sibling = m + 1 - 2 * core
    place = core * tiers + tier
    own_columns = pl.ds(pl.multiple_of(side * columns, 128), columns)
    twin_columns = pl.ds(pl.multiple_of((1 - side) * columns, 128), columns)
    own_half = pl.ds(core * tiers, tiers)
    sibling_half = pl.ds((1 - core) * tiers, tiers)
    at_home = spot == m

    def remote(source, target, send, recv, dp, mp):
        return pltpu.make_async_remote_copy(
            src_ref=source,
            dst_ref=target,
            send_sem=send,
            recv_sem=recv,
            device_id={"dp": dp, "mp": mp},
            device_id_type=pl.DeviceIdType.MESH,
        )

    def arrival(target, recv):
        return remote(target, target, weight_send.at[0], recv, d, m)

    def turn(index):
        low = 2 * spot < line
        above = line - 1 - spot
        first = jnp.where(low, above, spot)
        early = jnp.where(low, line - 1 - index, index)
        late = jnp.where(low, index - first, line - 1 - (index - first))
        return jnp.where(index >= line - 1, spot, jnp.where(index < first, early, late))

    def quarter(index):
        return grad_ref.at[pl.ds(pl.multiple_of(index * part, part), part), :]

    weight_copy = remote(
        weight_ref, weight_all.at[:, own_columns], weight_send.at[0], weight_recv.at[0], twin, m
    )
    weight_here = pltpu.make_async_copy(
        weight_ref, weight_all.at[:, own_columns], weight_recv.at[1]
    )

    def direct(step, c):
        target = lax.rem(tier + step, tiers)
        index = c * tiers + target
        return remote(
            quarter(index),
            grads.at[spot, index],
            swap_send.at[step, c],
            grad_recv.at[spot, index],
            2 * m + side,
            2 * target + c,
        )

    def stay():
        return pltpu.make_async_copy(quarter(place), grads.at[spot, place], grad_recv.at[spot, place])

    def relay(step, c):
        target = lax.rem(tier + step, tiers)
        return remote(
            quarter(c * tiers + target),
            relay_in.at[step, c],
            swap_send.at[step, c],
            relay_recv.at[step, c],
            d,
            2 * target + core,
        )

    def relay_origin(step):
        return 2 * lax.rem(tier + tiers - step, tiers) + core

    def onward(step, c):
        return remote(
            relay_in.at[step, c],
            grads.at[spot, c * tiers + tier],
            relay_send.at[step, c],
            grad_recv.at[spot, c * tiers + tier],
            2 * relay_origin(step) + side,
            2 * tier + c,
        )

    def swaps(act, local):
        for step in range(1, tiers):
            for c in range(2):
                @pl.when(at_home)
                def _(step=step, c=c):
                    act(direct(step, c))

                @pl.when(jnp.logical_not(at_home))
                def _(step=step, c=c):
                    act(relay(step, c))

        for c in range(2):
            mine = at_home & (core == c)

            @pl.when(mine)
            def _():
                local()

            @pl.when(jnp.logical_not(mine))
            def _(c=c):
                act(direct(0, c))

    swaps(lambda copy: copy.start(), lambda: stay().start())
    weight_copy.start()
    weight_here.start()

    allowed = allowed_pairs(lengths_ref, rows)
    for h in range(head_count):
        kv = h // group_size
        head = slice(h * HEAD_WIDTH, (h + 1) * HEAD_WIDTH)
        kv_head = slice(kv * HEAD_WIDTH, (kv + 1) * HEAD_WIDTH)
        logits = dot(query_ref[:, head], key_ref[:, kv_head], NT) * scale
        logits = jnp.where(allowed, logits, -jnp.inf)
        exp_terms = jnp.exp(logits - jnp.max(logits, axis=1, keepdims=True))
        probability = exp_terms / jnp.sum(exp_terms, axis=1, keepdims=True)
        probs[h] = probability
        heads_all[spot, :, head] = dot(
            probability.astype(jnp.bfloat16), value_ref[:, kv_head], NN
        ).astype(jnp.bfloat16)

    def heads_copy(block, way):
        return remote(
            heads_all.at[block],
            heads_all.at[block],
            heads_send.at[block, way],
            heads_recv.at[block],
            (d + 2, d - 2)[way],
            m,
        )

    def heads_pass(distance, started):
        for way, sign in ((0, -1), (1, 1)):
            block = spot + sign * distance
            target = spot - sign

            @pl.when((block >= 0) & (block < line))
            def _(block=block, way=way, target=target):
                if started and distance > 0:
                    arrival(heads_all.at[block], heads_recv.at[block]).wait_recv()

                @pl.when((target >= 0) & (target < line))
                def _():
                    if started:
                        heads_copy(block, way).start()
                    else:
                        heads_copy(block, way).wait_send()

    heads_pass(0, True)

    for step in range(1, tiers):
        for c in range(2):
            @pl.when(relay_origin(step) != spot)
            def _(step=step, c=c):
                arrival(relay_in.at[step, c], relay_recv.at[step, c]).wait_recv()
                onward(step, c).start()

    def lift(block, step):
        target = lax.rem(tier + step, tiers)
        return remote(
            grads.at[block, place],
            grads.at[block, place],
            lift_send.at[block, step],
            grad_recv.at[block, place],
            d,
            2 * target + core,
        )

    def lift_step(index, carry):
        block = turn(index)
        arrival(grads.at[block, place], grad_recv.at[block, place]).wait_recv()
        for step in range(1, tiers):
            lift(block, step).start()
        return carry

    lax.fori_loop(0, line, lift_step, 0)

    def layer_begin(block):
        layer_part[block] = dot(heads_all[block], weight_all[...], NN).astype(jnp.bfloat16).reshape(
            n_mp, part, span
        )
        pair_copy(block).start()
        turned = heads_all[block].astype(jnp.float32).T.astype(jnp.bfloat16)
        heads_turned[block] = turned

    def pair_copy(block):
        return remote(
            layer_part.at[block, sibling_half],
            pair_in.at[block],
            pair_send.at[block],
            pair_recv.at[block],
            d,
            sibling,
        )

    def tier_copy(block, step):
        target = lax.rem(tier + step, tiers)
        return remote(
            pair_out.at[block, step],
            tier_in.at[block, step],
            tier_send.at[block, step],
            tier_recv.at[block, step],
            d,
            2 * target + core,
        )

    def layer_pair(block):
        arrival(pair_in.at[block], pair_recv.at[block]).wait_recv()
        for step in range(1, tiers):
            target = lax.rem(tier + step, tiers)
            pair_out[block, step] = (
                layer_part[block, core * tiers + target].astype(jnp.float32)
                + pair_in[block, target].astype(jnp.float32)
            ).astype(jnp.bfloat16)
            tier_copy(block, step).start()

    def done_copy(block):
        return remote(
            layer_sum.at[block],
            layer_in.at[place],
            done_send.at[block],
            done_recv.at[place],
            2 * block + side,
            spot,
        )

    def layer_end(block):
        total = layer_part[block, place].astype(jnp.float32) + pair_in[block, tier].astype(
            jnp.float32
        )
        for step in range(1, tiers):
            arrival(tier_in.at[block, step], tier_recv.at[block, step]).wait_recv()
            total = total + tier_in[block, step].astype(jnp.float32)
        total = total.astype(jnp.bfloat16)
        here = at_home & (block == spot)

        @pl.when(here)
        def _():
            layer_in[place] = total

        @pl.when(jnp.logical_not(here))
        def _():
            layer_sum[block] = total
            done_copy(block).start()

    arrival(weight_all.at[:, twin_columns], weight_recv.at[0]).wait_recv()
    weight_here.wait()

    def side_copy(block):
        return remote(
            grads.at[block, own_half],
            grads.at[block, own_half],
            side_send.at[block],
            side_recv.at[block],
            d,
            sibling,
        )

    def layer_step(index, carry):
        layer_begin(turn(index))
        return carry

    lax.fori_loop(line - 1, line, layer_step, 0)
    heads_pass(1, True)

    def side_step(index, carry):
        block = turn(index)
        for step in range(1, tiers):
            from_place = core * tiers + lax.rem(tier + step, tiers)
            arrival(grads.at[block, from_place], grad_recv.at[block, from_place]).wait_recv()
        side_copy(block).start()
        return carry

    lax.fori_loop(0, line, side_step, 0)

    def up_copy(block, way):
        return remote(
            up_out.at[block],
            up_in.at[way, block],
            up_send.at[block],
            up_recv.at[way, block],
            (d + 2, d - 2)[way],
            m,
        )

    def up_block(index, carry):
        block = turn(index)
        arrival(grads.at[block, sibling_half], side_recv.at[block]).wait_recv()
        up_own[block] = dot(grads[block].reshape(rows, span), weight_all[...], NT)
        return carry

    def up_pass(index, started):
        block = turn(index)
        for way, sign in ((0, 1), (1, -1)):
            origin = spot - sign

            @pl.when((block - spot) * sign > 0)
            def _(way=way, origin=origin):
                if started:
                    inner = (origin >= 0) & (origin < line)

                    @pl.when(inner)
                    def _():
                        arrival(up_in.at[way, block], up_recv.at[way, block]).wait_recv()
                        up_out[block] = (
                            up_own[block] + up_in[way, block].astype(jnp.float32)
                        ).astype(jnp.bfloat16)

                    @pl.when(jnp.logical_not(inner))
                    def _():
                        up_out[block] = up_own[block].astype(jnp.bfloat16)

                    up_copy(block, way).start()
                else:
                    up_copy(block, way).wait_send()

    def up_step(index, carry):
        up_block(index, 0)

        @pl.when((spot == 0) | (spot == line - 1))
        def _():
            up_pass(index, True)

        return carry

    lax.fori_loop(0, line - 1, up_step, 0)
    up_block(line - 1, 0)

    def near(distance, act):
        for sign in (-1, 1):
            block = spot + sign * distance

            @pl.when((block >= 0) & (block < line))
            def _(block=block):
                act(block)

    layer_pair(spot)
    near(1, layer_begin)
    for distance in range(2, line):
        @pl.when((spot != 0) & (spot != line - 1))
        def _(distance=distance):
            up_pass(distance - 2, True)

        heads_pass(distance, True)
        near(distance - 1, layer_pair)
        near(distance, layer_begin)

    @pl.when((spot != 0) & (spot != line - 1))
    def _():
        up_pass(line - 2, True)

    near(line - 1, layer_pair)
    layer_end(spot)
    for distance in range(1, line):
        near(distance, layer_end)

    twin_copy = remote(twin_out, twin_in, twin_send.at[0], twin_recv.at[0], twin, m)

    def weight_half(which):
        total = dot(heads_turned[0], grads[0, :, :, which].reshape(rows, columns), NN)
        for block in range(1, line):
            total = total + dot(
                heads_turned[block], grads[block, :, :, which].reshape(rows, columns), NN
            )
        return total

    twin_out[...] = weight_half(twin_columns).astype(jnp.bfloat16)
    twin_copy.start()
    weight_grad_ref[...] = weight_half(own_columns)

    for way, sign in ((0, -1), (1, 1)):
        @pl.when((spot + sign >= 0) & (spot + sign < line))
        def _(way=way):
            arrival(up_in.at[way, spot], up_recv.at[way, spot]).wait_recv()
            up_own[spot] = up_own[spot] + up_in[way, spot].astype(jnp.float32)

    for h in range(head_count):
        kv = h // group_size
        head = slice(h * HEAD_WIDTH, (h + 1) * HEAD_WIDTH)
        kv_head = slice(kv * HEAD_WIDTH, (kv + 1) * HEAD_WIDTH)
        upstream = up_own[spot, :, head].astype(jnp.bfloat16)
        probability = probs[h]
        prob_grad = dot(upstream, value_ref[:, kv_head], NT)
        row_delta = jnp.sum(probability * prob_grad, axis=1, keepdims=True)
        score_grad = (probability * (prob_grad - row_delta) * scale).astype(jnp.bfloat16)
        query_grad_ref[:, head] = dot(score_grad, key_ref[:, kv_head], NN).astype(jnp.bfloat16)
        key_term = dot(score_grad, query_ref[:, head], TN)
        value_term = dot(probability.astype(jnp.bfloat16), upstream, TN)
        if h % group_size == 0:
            key_sum, value_sum = key_term, value_term
        else:
            key_sum, value_sum = key_sum + key_term, value_sum + value_term
        if h % group_size == group_size - 1:
            key_grad_ref[:, kv_head] = key_sum.astype(jnp.bfloat16)
            value_grad_ref[:, kv_head] = value_sum.astype(jnp.bfloat16)

    arrival(twin_in, twin_recv.at[0]).wait_recv()
    weight_grad_ref[...] += twin_in[...].astype(jnp.float32)

    for c in range(2):
        for level in range(tiers):
            @pl.when(jnp.logical_not(at_home & (place == c * tiers + level)))
            def _(index=c * tiers + level):
                arrival(layer_in.at[index], done_recv.at[index]).wait_recv()

    layer_ref[...] = layer_in[...].reshape(rows, span)

    swaps(lambda copy: copy.wait_send(), lambda: None)
    weight_copy.wait_send()
    for step in range(1, tiers):
        for c in range(2):
            @pl.when(relay_origin(step) != spot)
            def _(step=step, c=c):
                onward(step, c).wait_send()

    for distance in range(line - 1):
        heads_pass(distance, False)
    twin_copy.wait_send()

    def drain_step(block, carry):
        side_copy(block).wait_send()
        pair_copy(block).wait_send()
        for step in range(1, tiers):
            lift(block, step).wait_send()
            tier_copy(block, step).wait_send()

        @pl.when(jnp.logical_not(at_home & (block == spot)))
        def _():
            done_copy(block).wait_send()

        @pl.when(block < line - 1)
        def _():
            up_pass(block, False)

        return carry

    lax.fori_loop(0, line, drain_step, 0)


def fused(n_dp, n_mp, query_rows, key_rows, value_matrix, out_weight, out_grad, doc_lengths):
    rows, width = query_rows.shape
    columns = out_weight.shape[1]
    span = out_grad.shape[1]
    line = n_dp // 2
    tiers = n_mp // 2
    part = rows // n_mp
    vmem = pl.BlockSpec(memory_space=pltpu.VMEM)
    anywhere = pl.BlockSpec(memory_space=pl.ANY)
    dma = pltpu.SemaphoreType.DMA
    bf16 = jnp.bfloat16
    return pl.pallas_call(
        functools.partial(branch_kernel, n_dp, n_mp),
        out_shape=(
            jax.ShapeDtypeStruct(out_grad.shape, bf16),
            jax.ShapeDtypeStruct(query_rows.shape, bf16),
            jax.ShapeDtypeStruct(key_rows.shape, bf16),
            jax.ShapeDtypeStruct(value_matrix.shape, bf16),
            jax.ShapeDtypeStruct(out_weight.shape, jnp.float32),
        ),
        in_specs=[pl.BlockSpec(memory_space=pltpu.SMEM)] + [vmem] * 3 + [anywhere] * 2,
        out_specs=(vmem,) * 5,
        scratch_shapes=[
            pltpu.VMEM((width, span), bf16),
            pltpu.VMEM((line, n_mp, part, span), bf16),
            pltpu.VMEM((tiers, 2, part, span), bf16),
            pltpu.VMEM((line, rows, width), bf16),
            pltpu.VMEM((line, width, rows), bf16),
            pltpu.VMEM((line, rows, width), jnp.float32),
            pltpu.VMEM((2, line, rows, width), bf16),
            pltpu.VMEM((line, rows, width), bf16),
            pltpu.VMEM((line, n_mp, part, span), bf16),
            pltpu.VMEM((line, tiers, part, span), bf16),
            pltpu.VMEM((line, tiers, part, span), bf16),
            pltpu.VMEM((line, tiers, part, span), bf16),
            pltpu.VMEM((line, part, span), bf16),
            pltpu.VMEM((n_mp, part, span), bf16),
            pltpu.VMEM((width, columns), bf16),
            pltpu.VMEM((width, columns), bf16),
            pltpu.VMEM((width // HEAD_WIDTH, rows, rows), jnp.float32),
            dma((1,)),
            dma((2,)),
            dma((tiers, 2)),
            dma((tiers, 2)),
            dma((tiers, 2)),
            dma((line, n_mp)),
            dma((line, tiers)),
            dma((line,)),
            dma((line,)),
            dma((line, 2)),
            dma((line,)),
            dma((line,)),
            dma((2, line)),
            dma((line,)),
            dma((line,)),
            dma((line, tiers)),
            dma((line, tiers)),
            dma((line,)),
            dma((n_mp,)),
            dma((1,)),
            dma((1,)),
        ],
        compiler_params=pltpu.CompilerParams(
            has_side_effects=True, vmem_limit_bytes=60 * 1024 * 1024
        ),
    )(doc_lengths, query_rows, key_rows, value_matrix, out_weight, out_grad)


def body_of(n_dp, n_mp):
    def body(query_rows, key_rows, value_matrix, out_weight, out_grad, doc_lengths):
        arrays = (query_rows, key_rows, value_matrix, out_weight, out_grad, doc_lengths)
        columns = out_weight.shape[1]
        rows, width = query_rows.shape
        held = 2 * n_dp * rows * (4 * columns + 3 * width)
        if (
            columns % 128 == 0
            and rows % 128 == 0
            and rows % (16 * n_mp) == 0
            and n_dp == 2 * n_mp
            and n_mp % 2 == 0
            and n_mp > 2
            and 2 * columns == out_grad.shape[1]
            and held < 24 * 1024 * 1024
        ):
            return fused(n_dp, n_mp, *arrays)
        return per_device(*arrays)

    return body


def solution(mesh):
    placed = (
        P("dp", "mp"),
        P("dp", "mp"),
        P("dp", "mp"),
        P("mp", "dp"),
        P("dp", "mp"),
        P("dp", None),
    )
    return jax.shard_map(
        body_of(mesh.shape["dp"], mesh.shape["mp"]),
        mesh=mesh,
        in_specs=placed,
        out_specs=(P("dp", "mp"), P("dp", "mp"), P("dp", "mp"), P("dp", "mp"), P("mp", "dp")),
        check_vma=False,
    )
```

```python
import functools

import jax
import jax.numpy as jnp
from jax import lax
from jax.experimental import pallas as pl
from jax.experimental.pallas import tpu as pltpu
from jax.sharding import PartitionSpec as P

HEAD_WIDTH = 128
TILE = 128


def local_segments(lengths, row_count):
    segment_ends = jnp.cumsum(lengths)
    positions = jnp.arange(row_count, dtype=jnp.int32)
    return jnp.sum((positions[:, None] >= segment_ends[None, :]).astype(jnp.int32), axis=1)


def to_heads(matrix):
    return matrix.reshape(matrix.shape[0], matrix.shape[1] // HEAD_WIDTH, HEAD_WIDTH).transpose(
        1, 0, 2
    )


def from_heads(tensor):
    return tensor.transpose(1, 0, 2).reshape(tensor.shape[1], tensor.shape[0] * tensor.shape[2])


def attend(queries, key_rows, value_matrix, upstreams, segment):
    head_count, row_count, head_size = queries.shape
    tile_rows = min(TILE, row_count)
    block_count = row_count // tile_rows
    softmax_scale = HEAD_WIDTH ** (-0.5)
    offsets = jnp.arange(tile_rows, dtype=jnp.int32)
    empty_rows = jnp.zeros((tile_rows, head_size), jnp.float32)
    key_sums = [empty_rows] * block_count
    value_sums = [empty_rows] * block_count
    attended_blocks = []
    grad_blocks = []
    for block_index in range(block_count):
        row_start = block_index * tile_rows
        query_tile = queries[:, row_start : row_start + tile_rows]
        upstream_tile = upstreams[:, row_start : row_start + tile_rows]
        query_segment = segment[row_start : row_start + tile_rows]
        active = [
            segment[(column_index + 1) * tile_rows - 1] >= query_segment[0]
            for column_index in range(block_index + 1)
        ]
        score_tiles = []
        for column_index in range(block_index + 1):
            column_start = column_index * tile_rows
            key_tile = key_rows[column_start : column_start + tile_rows]
            key_segment = segment[column_start : column_start + tile_rows]
            allowed = (query_segment[:, None] == key_segment[None, :]) & (
                (row_start + offsets)[:, None] >= (column_start + offsets)[None, :]
            )

            def score_tile(query_tile=query_tile, key_tile=key_tile, allowed=allowed):
                logits = (
                    jnp.einsum(
                        "hid,jd->hij", query_tile, key_tile, preferred_element_type=jnp.float32
                    )
                    * softmax_scale
                )
                return jnp.where(allowed[None], logits, -jnp.inf)

            def masked_tile():
                return jnp.full((head_count, tile_rows, tile_rows), -jnp.inf, jnp.float32)

            score_tiles.append(lax.cond(active[column_index], score_tile, masked_tile))
        logits = jnp.concatenate(score_tiles, axis=-1)
        row_max = jnp.max(logits, axis=-1, keepdims=True)
        exp_terms = jnp.exp(logits - row_max)
        probability = exp_terms / jnp.sum(exp_terms, axis=-1, keepdims=True)
        weights = probability.astype(jnp.bfloat16)
        attended = jnp.zeros((head_count, tile_rows, head_size), jnp.float32)
        grad_tiles = []
        for column_index in range(block_index + 1):
            column_start = column_index * tile_rows
            value_tile = value_matrix[column_start : column_start + tile_rows]
            weight_tile = weights[:, :, column_start : column_start + tile_rows]

            def forward_tile(
                weight_tile=weight_tile, value_tile=value_tile, upstream_tile=upstream_tile
            ):
                return (
                    jnp.einsum(
                        "hij,jd->hid", weight_tile, value_tile, preferred_element_type=jnp.float32
                    ),
                    jnp.einsum(
                        "hid,jd->hij", upstream_tile, value_tile, preferred_element_type=jnp.float32
                    ),
                )

            def empty_pair():
                return (
                    jnp.zeros((head_count, tile_rows, head_size), jnp.float32),
                    jnp.zeros((head_count, tile_rows, tile_rows), jnp.float32),
                )

            contribution, prob_grad_tile = lax.cond(active[column_index], forward_tile, empty_pair)
            attended = attended + contribution
            grad_tiles.append(prob_grad_tile)
        prob_grad = jnp.concatenate(grad_tiles, axis=-1)
        row_delta = jnp.sum(probability * prob_grad, axis=-1, keepdims=True)
        score_grad = (probability * (prob_grad - row_delta) * softmax_scale).astype(jnp.bfloat16)
        query_sum = jnp.zeros((head_count, tile_rows, head_size), jnp.float32)
        for column_index in range(block_index + 1):
            column_start = column_index * tile_rows
            key_tile = key_rows[column_start : column_start + tile_rows]
            score_piece = score_grad[:, :, column_start : column_start + tile_rows]
            weight_tile = weights[:, :, column_start : column_start + tile_rows]

            def backward_tile(
                score_piece=score_piece,
                key_tile=key_tile,
                weight_tile=weight_tile,
                query_tile=query_tile,
                upstream_tile=upstream_tile,
            ):
                return (
                    jnp.einsum(
                        "hij,jd->hid", score_piece, key_tile, preferred_element_type=jnp.float32
                    ),
                    jnp.einsum(
                        "hij,hid->jd", score_piece, query_tile, preferred_element_type=jnp.float32
                    ),
                    jnp.einsum(
                        "hij,hid->jd",
                        weight_tile,
                        upstream_tile,
                        preferred_element_type=jnp.float32,
                    ),
                )

            def empty_triple():
                return (
                    jnp.zeros((head_count, tile_rows, head_size), jnp.float32),
                    empty_rows,
                    empty_rows,
                )

            query_part, key_part, value_part = lax.cond(
                active[column_index], backward_tile, empty_triple
            )
            query_sum = query_sum + query_part
            key_sums[column_index] = key_sums[column_index] + key_part
            value_sums[column_index] = value_sums[column_index] + value_part
        attended_blocks.append(attended.astype(jnp.bfloat16))
        grad_blocks.append(query_sum.astype(jnp.bfloat16))
    return (
        jnp.concatenate(attended_blocks, axis=1),
        jnp.concatenate(grad_blocks, axis=1),
        jnp.concatenate(key_sums, axis=0),
        jnp.concatenate(value_sums, axis=0),
    )


def grad_term(grad_full, attended_heads):
    attended_flat = from_heads(attended_heads)
    return lax.dot_general(
        grad_full, attended_flat, (((0,), (0,)), ((), ())), preferred_element_type=jnp.float32
    )


def per_device(query_rows, key_rows, value_matrix, out_weight, out_grad, doc_lengths):
    row_count = query_rows.shape[0]
    weight_full = lax.all_gather(out_weight, "dp", axis=1, tiled=True)
    grad_full = lax.all_gather(out_grad, "mp", axis=1, tiled=True)
    attn_grad = lax.dot_general(
        grad_full, weight_full, (((1,), (1,)), ((), ())), preferred_element_type=jnp.float32
    ).astype(jnp.bfloat16)
    segment = local_segments(doc_lengths[0], row_count)
    queries = to_heads(query_rows)
    upstreams = to_heads(attn_grad)
    attended, query_grad, key_sum, value_sum = attend(
        queries, key_rows, value_matrix, upstreams, segment
    )
    key_grad = key_sum.astype(jnp.bfloat16)
    value_grad = value_sum.astype(jnp.bfloat16)
    weight_part = lax.psum_scatter(
        grad_term(grad_full, attended), "dp", scatter_dimension=0, tiled=True
    )
    attended_flat = from_heads(attended)
    query_grad = from_heads(query_grad)
    partial_sum = jnp.dot(attended_flat, weight_full, preferred_element_type=jnp.float32).astype(
        jnp.bfloat16
    )
    layer_out = lax.psum_scatter(
        lax.optimization_barrier(partial_sum).astype(jnp.float32).astype(jnp.bfloat16),
        "mp",
        scatter_dimension=1,
        tiled=True,
    )
    return (layer_out, query_grad, key_grad, value_grad, weight_part.T)


def dot(a, b, dims):
    return lax.dot_general(a, b, (dims, ((), ())), preferred_element_type=jnp.float32)


NN = ((1,), (0,))
NT = ((1,), (1,))
TN = ((0,), (0,))


def allowed_pairs(lengths_ref, rows):
    row_at = lax.broadcasted_iota(jnp.int32, (rows, 1), 0)
    column_at = lax.broadcasted_iota(jnp.int32, (1, rows), 1)
    row_segment = jnp.zeros((rows, 1), jnp.int32)
    column_segment = jnp.zeros((1, rows), jnp.int32)
    end = jnp.int32(0)
    for index in range(lengths_ref.shape[1]):
        end = end + lengths_ref[0, index]
        row_segment = row_segment + jnp.where(row_at >= end, 1, 0)
        column_segment = column_segment + jnp.where(column_at >= end, 1, 0)
    return (row_segment == column_segment) & (row_at >= column_at)


def branch_kernel(
    n_dp,
    n_mp,
    lengths_ref,
    query_ref,
    key_ref,
    value_ref,
    weight_ref,
    grad_ref,
    layer_ref,
    query_grad_ref,
    key_grad_ref,
    value_grad_ref,
    weight_grad_ref,
    weight_all,
    grads,
    relay_in,
    heads_all,
    heads_turned,
    up_own,
    up_in,
    up_out,
    layer_part,
    pair_in,
    pair_out,
    tier_in,
    layer_sum,
    layer_in,
    twin_out,
    twin_in,
    probs,
    weight_send,
    weight_recv,
    swap_send,
    relay_send,
    relay_recv,
    grad_recv,
    lift_send,
    side_send,
    side_recv,
    heads_send,
    heads_recv,
    up_send,
    up_recv,
    pair_send,
    pair_recv,
    tier_send,
    tier_recv,
    done_send,
    done_recv,
    twin_send,
    twin_recv,
):
    d = lax.axis_index("dp")
    m = lax.axis_index("mp")
    line = n_dp // 2
    tiers = n_mp // 2
    rows = query_ref.shape[0]
    part = rows // n_mp
    width = query_ref.shape[1]
    columns = weight_ref.shape[1]
    span = grad_ref.shape[1]
    head_count = width // HEAD_WIDTH
    group_size = width // key_ref.shape[1]
    scale = HEAD_WIDTH ** (-0.5)
    spot = lax.div(d, 2)
    side = lax.rem(d, 2)
    twin = d + 1 - 2 * side
    core = lax.rem(m, 2)
    tier = lax.div(m, 2)
    sibling = m + 1 - 2 * core
    place = core * tiers + tier
    own_columns = pl.ds(pl.multiple_of(side * columns, 128), columns)
    twin_columns = pl.ds(pl.multiple_of((1 - side) * columns, 128), columns)
    own_half = pl.ds(core * tiers, tiers)
    sibling_half = pl.ds((1 - core) * tiers, tiers)
    at_home = spot == m

    def remote(source, target, send, recv, dp, mp):
        return pltpu.make_async_remote_copy(
            src_ref=source,
            dst_ref=target,
            send_sem=send,
            recv_sem=recv,
            device_id={"dp": dp, "mp": mp},
            device_id_type=pl.DeviceIdType.MESH,
        )

    def arrival(target, recv):
        return remote(target, target, weight_send.at[0], recv, d, m)

    def turn(index):
        low = 2 * spot < line
        above = line - 1 - spot
        first = jnp.where(low, above, spot)
        early = jnp.where(low, line - 1 - index, index)
        late = jnp.where(low, index - first, line - 1 - (index - first))
        return jnp.where(index < first, early, late)

    def quarter(index):
        return grad_ref.at[pl.ds(pl.multiple_of(index * part, part), part), :]

    weight_copy = remote(
        weight_ref, weight_all.at[:, own_columns], weight_send.at[0], weight_recv.at[0], twin, m
    )
    weight_here = pltpu.make_async_copy(
        weight_ref, weight_all.at[:, own_columns], weight_recv.at[1]
    )

    def direct(step, c):
        target = lax.rem(tier + step, tiers)
        index = c * tiers + target
        return remote(
            quarter(index),
            grads.at[spot, index],
            swap_send.at[step, c],
            grad_recv.at[spot, index],
            2 * m + side,
            2 * target + c,
        )

    def stay():
        return pltpu.make_async_copy(quarter(place), grads.at[spot, place], grad_recv.at[spot, place])

    def relay(step, c):
        target = lax.rem(tier + step, tiers)
        return remote(
            quarter(c * tiers + target),
            relay_in.at[step, c],
            swap_send.at[step, c],
            relay_recv.at[step, c],
            d,
            2 * target + core,
        )

    def relay_origin(step):
        return 2 * lax.rem(tier + tiers - step, tiers) + core

    def onward(step, c):
        return remote(
            relay_in.at[step, c],
            grads.at[spot, c * tiers + tier],
            relay_send.at[step, c],
            grad_recv.at[spot, c * tiers + tier],
            2 * relay_origin(step) + side,
            2 * tier + c,
        )

    def swaps(act, local):
        for step in range(1, tiers):
            for c in range(2):
                @pl.when(at_home)
                def _(step=step, c=c):
                    act(direct(step, c))

                @pl.when(jnp.logical_not(at_home))
                def _(step=step, c=c):
                    act(relay(step, c))

        for c in range(2):
            mine = at_home & (core == c)

            @pl.when(mine)
            def _():
                local()

            @pl.when(jnp.logical_not(mine))
            def _(c=c):
                act(direct(0, c))

    swaps(lambda copy: copy.start(), lambda: stay().start())
    weight_copy.start()
    weight_here.start()

    allowed = allowed_pairs(lengths_ref, rows)
    for h in range(head_count):
        kv = h // group_size
        head = slice(h * HEAD_WIDTH, (h + 1) * HEAD_WIDTH)
        kv_head = slice(kv * HEAD_WIDTH, (kv + 1) * HEAD_WIDTH)
        logits = dot(query_ref[:, head], key_ref[:, kv_head], NT) * scale
        logits = jnp.where(allowed, logits, -jnp.inf)
        exp_terms = jnp.exp(logits - jnp.max(logits, axis=1, keepdims=True))
        probability = exp_terms / jnp.sum(exp_terms, axis=1, keepdims=True)
        probs[h] = probability
        heads_all[spot, :, head] = dot(
            probability.astype(jnp.bfloat16), value_ref[:, kv_head], NN
        ).astype(jnp.bfloat16)

    def heads_copy(block, way):
        return remote(
            heads_all.at[block],
            heads_all.at[block],
            heads_send.at[block, way],
            heads_recv.at[block],
            (d + 2, d - 2)[way],
            m,
        )

    def heads_pass(distance, started):
        for way, sign in ((0, -1), (1, 1)):
            block = spot + sign * distance
            target = spot - sign

            @pl.when((block >= 0) & (block < line))
            def _(block=block, way=way, target=target):
                if started and distance > 0:
                    arrival(heads_all.at[block], heads_recv.at[block]).wait_recv()

                @pl.when((target >= 0) & (target < line))
                def _():
                    if started:
                        heads_copy(block, way).start()
                    else:
                        heads_copy(block, way).wait_send()

    heads_pass(0, True)

    def lift(block, step):
        target = lax.rem(tier + step, tiers)
        return remote(
            grads.at[block, place],
            grads.at[block, place],
            lift_send.at[block, step],
            grad_recv.at[block, place],
            d,
            2 * target + core,
        )

    def near(distance, act):
        if distance == 0:
            act(spot)
        else:
            for sign in (-1, 1):
                block = spot + sign * distance

                @pl.when((block >= 0) & (block < line))
                def _(block=block):
                    act(block)

    def lift_begin(block):
        arrival(grads.at[block, place], grad_recv.at[block, place]).wait_recv()
        for step in range(1, tiers):
            lift(block, step).start()

    near(0, lift_begin)
    for step in range(1, tiers):
        for c in range(2):
            @pl.when(relay_origin(step) != spot)
            def _(step=step, c=c):
                arrival(relay_in.at[step, c], relay_recv.at[step, c]).wait_recv()
                onward(step, c).start()

    near(1, lift_begin)
    heads_pass(1, True)
    for distance in range(2, line):
        near(distance, lift_begin)

    def layer_begin(block):
        layer_part[block] = dot(heads_all[block], weight_all[...], NN).astype(jnp.bfloat16).reshape(
            n_mp, part, span
        )
        pair_copy(block).start()
        turned = heads_all[block].astype(jnp.float32).T.astype(jnp.bfloat16)
        heads_turned[block] = turned

    def pair_copy(block):
        return remote(
            layer_part.at[block, sibling_half],
            pair_in.at[block],
            pair_send.at[block],
            pair_recv.at[block],
            d,
            sibling,
        )

    def tier_copy(block, step):
        target = lax.rem(tier + step, tiers)
        return remote(
            pair_out.at[block, step],
            tier_in.at[block, step],
            tier_send.at[block, step],
            tier_recv.at[block, step],
            d,
            2 * target + core,
        )

    def layer_pair(block):
        arrival(pair_in.at[block], pair_recv.at[block]).wait_recv()
        for step in range(1, tiers):
            target = lax.rem(tier + step, tiers)
            pair_out[block, step] = (
                layer_part[block, core * tiers + target].astype(jnp.float32)
                + pair_in[block, target].astype(jnp.float32)
            ).astype(jnp.bfloat16)
            tier_copy(block, step).start()

    def done_copy(block):
        return remote(
            layer_sum.at[block],
            layer_in.at[place],
            done_send.at[block],
            done_recv.at[place],
            2 * block + side,
            spot,
        )

    def layer_end(block):
        total = layer_part[block, place].astype(jnp.float32) + pair_in[block, tier].astype(
            jnp.float32
        )
        for step in range(1, tiers):
            arrival(tier_in.at[block, step], tier_recv.at[block, step]).wait_recv()
            total = total + tier_in[block, step].astype(jnp.float32)
        total = total.astype(jnp.bfloat16)
        here = at_home & (block == spot)

        @pl.when(here)
        def _():
            layer_in[place] = total

        @pl.when(jnp.logical_not(here))
        def _():
            layer_sum[block] = total
            done_copy(block).start()

    def side_copy(block):
        return remote(
            grads.at[block, own_half],
            grads.at[block, own_half],
            side_send.at[block],
            side_recv.at[block],
            d,
            sibling,
        )

    def side_begin(block):
        for step in range(1, tiers):
            from_place = core * tiers + lax.rem(tier + step, tiers)
            arrival(grads.at[block, from_place], grad_recv.at[block, from_place]).wait_recv()
        side_copy(block).start()

    def up_copy(block, way):
        return remote(
            up_out.at[block],
            up_in.at[way, block],
            up_send.at[block],
            up_recv.at[way, block],
            (d + 2, d - 2)[way],
            m,
        )

    def up_block(block):
        arrival(grads.at[block, sibling_half], side_recv.at[block]).wait_recv()
        up_own[block] = dot(grads[block].reshape(rows, span), weight_all[...], NT)

    def up_pass(index, started):
        block = turn(index)
        for way, sign in ((0, 1), (1, -1)):
            origin = spot - sign

            @pl.when((block - spot) * sign > 0)
            def _(way=way, origin=origin):
                if started:
                    inner = (origin >= 0) & (origin < line)

                    @pl.when(inner)
                    def _():
                        arrival(up_in.at[way, block], up_recv.at[way, block]).wait_recv()
                        up_out[block] = (
                            up_own[block] + up_in[way, block].astype(jnp.float32)
                        ).astype(jnp.bfloat16)

                    @pl.when(jnp.logical_not(inner))
                    def _():
                        up_out[block] = up_own[block].astype(jnp.bfloat16)

                    up_copy(block, way).start()
                else:
                    up_copy(block, way).wait_send()

    twin_copy = remote(twin_out, twin_in, twin_send.at[0], twin_recv.at[0], twin, m)

    def weight_half(which):
        total = dot(heads_turned[0], grads[0, :, :, which].reshape(rows, columns), NN)
        for block in range(1, line):
            total = total + dot(
                heads_turned[block], grads[block, :, :, which].reshape(rows, columns), NN
            )
        return total

    arrival(weight_all.at[:, twin_columns], weight_recv.at[0]).wait_recv()
    weight_here.wait()
    layer_begin(spot)
    near(0, side_begin)
    near(1, side_begin)
    near(0, up_block)
    heads_pass(2, True)
    for distance in range(2, line):
        near(distance, side_begin)
        near(distance - 1, up_block)
    near(line - 1, up_block)
    edge = (spot == 0) | (spot == line - 1)

    def up_turn(index):
        @pl.when(jnp.logical_not(edge))
        def _():
            up_pass(index, True)

    def edge_step(index, carry):
        up_pass(index, True)
        return carry

    @pl.when(edge)
    def _():
        lax.fori_loop(0, line - 1, edge_step, 0)

    near(0, layer_pair)
    near(1, layer_begin)
    for distance in range(2, line - 1):
        near(distance - 1, layer_pair)
        near(distance, layer_begin)
        if distance > 2:
            heads_pass(distance, True)
    for index in range(line - 2):
        up_turn(index)
        if index == 0:
            heads_pass(line - 1, True)
            near(line - 2, layer_pair)
            near(line - 1, layer_begin)
    twin_out[...] = weight_half(twin_columns).astype(jnp.bfloat16)
    twin_copy.start()
    near(line - 1, layer_pair)
    near(0, layer_end)
    up_turn(line - 2)
    for distance in range(1, line):
        near(distance, layer_end)
    weight_grad_ref[...] = weight_half(own_columns)

    for way, sign in ((0, -1), (1, 1)):
        @pl.when((spot + sign >= 0) & (spot + sign < line))
        def _(way=way):
            arrival(up_in.at[way, spot], up_recv.at[way, spot]).wait_recv()
            up_own[spot] = up_own[spot] + up_in[way, spot].astype(jnp.float32)

    for h in range(head_count):
        kv = h // group_size
        head = slice(h * HEAD_WIDTH, (h + 1) * HEAD_WIDTH)
        kv_head = slice(kv * HEAD_WIDTH, (kv + 1) * HEAD_WIDTH)
        upstream = up_own[spot, :, head].astype(jnp.bfloat16)
        probability = probs[h]
        prob_grad = dot(upstream, value_ref[:, kv_head], NT)
        row_delta = jnp.sum(probability * prob_grad, axis=1, keepdims=True)
        score_grad = (probability * (prob_grad - row_delta) * scale).astype(jnp.bfloat16)
        query_grad_ref[:, head] = dot(score_grad, key_ref[:, kv_head], NN).astype(jnp.bfloat16)
        key_term = dot(score_grad, query_ref[:, head], TN)
        value_term = dot(probability.astype(jnp.bfloat16), upstream, TN)
        if h % group_size == 0:
            key_sum, value_sum = key_term, value_term
        else:
            key_sum, value_sum = key_sum + key_term, value_sum + value_term
        if h % group_size == group_size - 1:
            key_grad_ref[:, kv_head] = key_sum.astype(jnp.bfloat16)
            value_grad_ref[:, kv_head] = value_sum.astype(jnp.bfloat16)

    arrival(twin_in, twin_recv.at[0]).wait_recv()
    weight_grad_ref[...] += twin_in[...].astype(jnp.float32)

    for c in range(2):
        for level in range(tiers):
            @pl.when(jnp.logical_not(at_home & (place == c * tiers + level)))
            def _(index=c * tiers + level):
                arrival(layer_in.at[index], done_recv.at[index]).wait_recv()

    layer_ref[...] = layer_in[...].reshape(rows, span)

    swaps(lambda copy: copy.wait_send(), lambda: None)
    weight_copy.wait_send()
    for step in range(1, tiers):
        for c in range(2):
            @pl.when(relay_origin(step) != spot)
            def _(step=step, c=c):
                onward(step, c).wait_send()

    for distance in range(line - 1):
        heads_pass(distance, False)
    twin_copy.wait_send()

    def drain_step(block, carry):
        side_copy(block).wait_send()
        pair_copy(block).wait_send()
        for step in range(1, tiers):
            lift(block, step).wait_send()
            tier_copy(block, step).wait_send()

        @pl.when(jnp.logical_not(at_home & (block == spot)))
        def _():
            done_copy(block).wait_send()

        @pl.when(block < line - 1)
        def _():
            up_pass(block, False)

        return carry

    lax.fori_loop(0, line, drain_step, 0)


def fused(n_dp, n_mp, query_rows, key_rows, value_matrix, out_weight, out_grad, doc_lengths):
    rows, width = query_rows.shape
    columns = out_weight.shape[1]
    span = out_grad.shape[1]
    line = n_dp // 2
    tiers = n_mp // 2
    part = rows // n_mp
    vmem = pl.BlockSpec(memory_space=pltpu.VMEM)
    anywhere = pl.BlockSpec(memory_space=pl.ANY)
    dma = pltpu.SemaphoreType.DMA
    bf16 = jnp.bfloat16
    return pl.pallas_call(
        functools.partial(branch_kernel, n_dp, n_mp),
        out_shape=(
            jax.ShapeDtypeStruct(out_grad.shape, bf16),
            jax.ShapeDtypeStruct(query_rows.shape, bf16),
            jax.ShapeDtypeStruct(key_rows.shape, bf16),
            jax.ShapeDtypeStruct(value_matrix.shape, bf16),
            jax.ShapeDtypeStruct(out_weight.shape, jnp.float32),
        ),
        in_specs=[pl.BlockSpec(memory_space=pltpu.SMEM)] + [vmem] * 3 + [anywhere] * 2,
        out_specs=(vmem,) * 5,
        scratch_shapes=[
            pltpu.VMEM((width, span), bf16),
            pltpu.VMEM((line, n_mp, part, span), bf16),
            pltpu.VMEM((tiers, 2, part, span), bf16),
            pltpu.VMEM((line, rows, width), bf16),
            pltpu.VMEM((line, width, rows), bf16),
            pltpu.VMEM((line, rows, width), jnp.float32),
            pltpu.VMEM((2, line, rows, width), bf16),
            pltpu.VMEM((line, rows, width), bf16),
            pltpu.VMEM((line, n_mp, part, span), bf16),
            pltpu.VMEM((line, tiers, part, span), bf16),
            pltpu.VMEM((line, tiers, part, span), bf16),
            pltpu.VMEM((line, tiers, part, span), bf16),
            pltpu.VMEM((line, part, span), bf16),
            pltpu.VMEM((n_mp, part, span), bf16),
            pltpu.VMEM((width, columns), bf16),
            pltpu.VMEM((width, columns), bf16),
            pltpu.VMEM((width // HEAD_WIDTH, rows, rows), jnp.float32),
            dma((1,)),
            dma((2,)),
            dma((tiers, 2)),
            dma((tiers, 2)),
            dma((tiers, 2)),
            dma((line, n_mp)),
            dma((line, tiers)),
            dma((line,)),
            dma((line,)),
            dma((line, 2)),
            dma((line,)),
            dma((line,)),
            dma((2, line)),
            dma((line,)),
            dma((line,)),
            dma((line, tiers)),
            dma((line, tiers)),
            dma((line,)),
            dma((n_mp,)),
            dma((1,)),
            dma((1,)),
        ],
        compiler_params=pltpu.CompilerParams(
            has_side_effects=True, vmem_limit_bytes=36 * 1024 * 1024
        ),
    )(doc_lengths, query_rows, key_rows, value_matrix, out_weight, out_grad)


def body_of(n_dp, n_mp):
    def body(query_rows, key_rows, value_matrix, out_weight, out_grad, doc_lengths):
        arrays = (query_rows, key_rows, value_matrix, out_weight, out_grad, doc_lengths)
        columns = out_weight.shape[1]
        rows, width = query_rows.shape
        held = 2 * n_dp * rows * (4 * columns + 3 * width)
        if (
            columns % 128 == 0
            and rows % 128 == 0
            and rows % (16 * n_mp) == 0
            and n_dp == 2 * n_mp
            and n_mp % 2 == 0
            and n_mp > 2
            and 2 * columns == out_grad.shape[1]
            and held < 24 * 1024 * 1024
        ):
            return fused(n_dp, n_mp, *arrays)
        return per_device(*arrays)

    return body


def solution(mesh):
    placed = (
        P("dp", "mp"),
        P("dp", "mp"),
        P("dp", "mp"),
        P("mp", "dp"),
        P("dp", "mp"),
        P("dp", None),
    )
    return jax.shard_map(
        body_of(mesh.shape["dp"], mesh.shape["mp"]),
        mesh=mesh,
        in_specs=placed,
        out_specs=(P("dp", "mp"), P("dp", "mp"), P("dp", "mp"), P("dp", "mp"), P("mp", "dp")),
        check_vma=False,
    )
```

```python
import functools

import jax
import jax.numpy as jnp
from jax import lax
from jax.experimental import pallas as pl
from jax.experimental.pallas import tpu as pltpu
from jax.sharding import PartitionSpec as P

HEAD_WIDTH = 128
TILE = 128


def local_segments(lengths, row_count):
    segment_ends = jnp.cumsum(lengths)
    positions = jnp.arange(row_count, dtype=jnp.int32)
    return jnp.sum((positions[:, None] >= segment_ends[None, :]).astype(jnp.int32), axis=1)


def to_heads(matrix):
    return matrix.reshape(matrix.shape[0], matrix.shape[1] // HEAD_WIDTH, HEAD_WIDTH).transpose(
        1, 0, 2
    )


def from_heads(tensor):
    return tensor.transpose(1, 0, 2).reshape(tensor.shape[1], tensor.shape[0] * tensor.shape[2])


def attend(queries, key_rows, value_matrix, upstreams, segment):
    head_count, row_count, head_size = queries.shape
    tile_rows = min(TILE, row_count)
    block_count = row_count // tile_rows
    softmax_scale = HEAD_WIDTH ** (-0.5)
    offsets = jnp.arange(tile_rows, dtype=jnp.int32)
    empty_rows = jnp.zeros((tile_rows, head_size), jnp.float32)
    key_sums = [empty_rows] * block_count
    value_sums = [empty_rows] * block_count
    attended_blocks = []
    grad_blocks = []
    for block_index in range(block_count):
        row_start = block_index * tile_rows
        query_tile = queries[:, row_start : row_start + tile_rows]
        upstream_tile = upstreams[:, row_start : row_start + tile_rows]
        query_segment = segment[row_start : row_start + tile_rows]
        active = [
            segment[(column_index + 1) * tile_rows - 1] >= query_segment[0]
            for column_index in range(block_index + 1)
        ]
        score_tiles = []
        for column_index in range(block_index + 1):
            column_start = column_index * tile_rows
            key_tile = key_rows[column_start : column_start + tile_rows]
            key_segment = segment[column_start : column_start + tile_rows]
            allowed = (query_segment[:, None] == key_segment[None, :]) & (
                (row_start + offsets)[:, None] >= (column_start + offsets)[None, :]
            )

            def score_tile(query_tile=query_tile, key_tile=key_tile, allowed=allowed):
                logits = (
                    jnp.einsum(
                        "hid,jd->hij", query_tile, key_tile, preferred_element_type=jnp.float32
                    )
                    * softmax_scale
                )
                return jnp.where(allowed[None], logits, -jnp.inf)

            def masked_tile():
                return jnp.full((head_count, tile_rows, tile_rows), -jnp.inf, jnp.float32)

            score_tiles.append(lax.cond(active[column_index], score_tile, masked_tile))
        logits = jnp.concatenate(score_tiles, axis=-1)
        row_max = jnp.max(logits, axis=-1, keepdims=True)
        exp_terms = jnp.exp(logits - row_max)
        probability = exp_terms / jnp.sum(exp_terms, axis=-1, keepdims=True)
        weights = probability.astype(jnp.bfloat16)
        attended = jnp.zeros((head_count, tile_rows, head_size), jnp.float32)
        grad_tiles = []
        for column_index in range(block_index + 1):
            column_start = column_index * tile_rows
            value_tile = value_matrix[column_start : column_start + tile_rows]
            weight_tile = weights[:, :, column_start : column_start + tile_rows]

            def forward_tile(
                weight_tile=weight_tile, value_tile=value_tile, upstream_tile=upstream_tile
            ):
                return (
                    jnp.einsum(
                        "hij,jd->hid", weight_tile, value_tile, preferred_element_type=jnp.float32
                    ),
                    jnp.einsum(
                        "hid,jd->hij", upstream_tile, value_tile, preferred_element_type=jnp.float32
                    ),
                )

            def empty_pair():
                return (
                    jnp.zeros((head_count, tile_rows, head_size), jnp.float32),
                    jnp.zeros((head_count, tile_rows, tile_rows), jnp.float32),
                )

            contribution, prob_grad_tile = lax.cond(active[column_index], forward_tile, empty_pair)
            attended = attended + contribution
            grad_tiles.append(prob_grad_tile)
        prob_grad = jnp.concatenate(grad_tiles, axis=-1)
        row_delta = jnp.sum(probability * prob_grad, axis=-1, keepdims=True)
        score_grad = (probability * (prob_grad - row_delta) * softmax_scale).astype(jnp.bfloat16)
        query_sum = jnp.zeros((head_count, tile_rows, head_size), jnp.float32)
        for column_index in range(block_index + 1):
            column_start = column_index * tile_rows
            key_tile = key_rows[column_start : column_start + tile_rows]
            score_piece = score_grad[:, :, column_start : column_start + tile_rows]
            weight_tile = weights[:, :, column_start : column_start + tile_rows]

            def backward_tile(
                score_piece=score_piece,
                key_tile=key_tile,
                weight_tile=weight_tile,
                query_tile=query_tile,
                upstream_tile=upstream_tile,
            ):
                return (
                    jnp.einsum(
                        "hij,jd->hid", score_piece, key_tile, preferred_element_type=jnp.float32
                    ),
                    jnp.einsum(
                        "hij,hid->jd", score_piece, query_tile, preferred_element_type=jnp.float32
                    ),
                    jnp.einsum(
                        "hij,hid->jd",
                        weight_tile,
                        upstream_tile,
                        preferred_element_type=jnp.float32,
                    ),
                )

            def empty_triple():
                return (
                    jnp.zeros((head_count, tile_rows, head_size), jnp.float32),
                    empty_rows,
                    empty_rows,
                )

            query_part, key_part, value_part = lax.cond(
                active[column_index], backward_tile, empty_triple
            )
            query_sum = query_sum + query_part
            key_sums[column_index] = key_sums[column_index] + key_part
            value_sums[column_index] = value_sums[column_index] + value_part
        attended_blocks.append(attended.astype(jnp.bfloat16))
        grad_blocks.append(query_sum.astype(jnp.bfloat16))
    return (
        jnp.concatenate(attended_blocks, axis=1),
        jnp.concatenate(grad_blocks, axis=1),
        jnp.concatenate(key_sums, axis=0),
        jnp.concatenate(value_sums, axis=0),
    )


def grad_term(grad_full, attended_heads):
    attended_flat = from_heads(attended_heads)
    return lax.dot_general(
        grad_full, attended_flat, (((0,), (0,)), ((), ())), preferred_element_type=jnp.float32
    )


def per_device(query_rows, key_rows, value_matrix, out_weight, out_grad, doc_lengths):
    row_count = query_rows.shape[0]
    weight_full = lax.all_gather(out_weight, "dp", axis=1, tiled=True)
    grad_full = lax.all_gather(out_grad, "mp", axis=1, tiled=True)
    attn_grad = lax.dot_general(
        grad_full, weight_full, (((1,), (1,)), ((), ())), preferred_element_type=jnp.float32
    ).astype(jnp.bfloat16)
    segment = local_segments(doc_lengths[0], row_count)
    queries = to_heads(query_rows)
    upstreams = to_heads(attn_grad)
    attended, query_grad, key_sum, value_sum = attend(
        queries, key_rows, value_matrix, upstreams, segment
    )
    key_grad = key_sum.astype(jnp.bfloat16)
    value_grad = value_sum.astype(jnp.bfloat16)
    weight_part = lax.psum_scatter(
        grad_term(grad_full, attended), "dp", scatter_dimension=0, tiled=True
    )
    attended_flat = from_heads(attended)
    query_grad = from_heads(query_grad)
    partial_sum = jnp.dot(attended_flat, weight_full, preferred_element_type=jnp.float32).astype(
        jnp.bfloat16
    )
    layer_out = lax.psum_scatter(
        lax.optimization_barrier(partial_sum).astype(jnp.float32).astype(jnp.bfloat16),
        "mp",
        scatter_dimension=1,
        tiled=True,
    )
    return (layer_out, query_grad, key_grad, value_grad, weight_part.T)


def dot(a, b, dims):
    return lax.dot_general(a, b, (dims, ((), ())), preferred_element_type=jnp.float32)


NN = ((1,), (0,))
NT = ((1,), (1,))
TN = ((0,), (0,))


def allowed_pairs(lengths_ref, rows):
    row_at = lax.broadcasted_iota(jnp.int32, (rows, 1), 0)
    column_at = lax.broadcasted_iota(jnp.int32, (1, rows), 1)
    row_segment = jnp.zeros((rows, 1), jnp.int32)
    column_segment = jnp.zeros((1, rows), jnp.int32)
    end = jnp.int32(0)
    for index in range(lengths_ref.shape[1]):
        end = end + lengths_ref[0, index]
        row_segment = row_segment + jnp.where(row_at >= end, 1, 0)
        column_segment = column_segment + jnp.where(column_at >= end, 1, 0)
    return (row_segment == column_segment) & (row_at >= column_at)


def branch_kernel(
    n_dp,
    n_mp,
    lengths_hbm,
    query_hbm,
    key_hbm,
    value_hbm,
    weight_ref,
    grad_ref,
    layer_ref,
    query_grad_ref,
    key_grad_ref,
    value_grad_ref,
    weight_grad_ref,
    lengths_ref,
    query_ref,
    key_ref,
    value_ref,
    weight_all,
    grads,
    relay_in,
    heads_all,
    heads_turned,
    up_own,
    up_in,
    up_out,
    layer_part,
    pair_in,
    pair_out,
    tier_in,
    layer_sum,
    layer_in,
    twin_out,
    twin_in,
    probs,
    weight_send,
    weight_recv,
    swap_send,
    relay_send,
    relay_recv,
    grad_recv,
    lift_send,
    side_send,
    side_recv,
    heads_send,
    heads_recv,
    up_send,
    up_recv,
    pair_send,
    pair_recv,
    tier_send,
    tier_recv,
    done_send,
    done_recv,
    twin_send,
    twin_recv,
    load_recv,
):
    d = lax.axis_index("dp")
    m = lax.axis_index("mp")
    line = n_dp // 2
    tiers = n_mp // 2
    rows = query_ref.shape[0]
    part = rows // n_mp
    width = query_ref.shape[1]
    columns = weight_ref.shape[1]
    span = grad_ref.shape[1]
    head_count = width // HEAD_WIDTH
    group_size = width // key_ref.shape[1]
    scale = HEAD_WIDTH ** (-0.5)
    spot = lax.div(d, 2)
    side = lax.rem(d, 2)
    twin = d + 1 - 2 * side
    core = lax.rem(m, 2)
    tier = lax.div(m, 2)
    sibling = m + 1 - 2 * core
    place = core * tiers + tier
    own_columns = pl.ds(pl.multiple_of(side * columns, 128), columns)
    twin_columns = pl.ds(pl.multiple_of((1 - side) * columns, 128), columns)
    own_half = pl.ds(core * tiers, tiers)
    sibling_half = pl.ds((1 - core) * tiers, tiers)
    at_home = spot == m

    def remote(source, target, send, recv, dp, mp):
        return pltpu.make_async_remote_copy(
            src_ref=source,
            dst_ref=target,
            send_sem=send,
            recv_sem=recv,
            device_id={"dp": dp, "mp": mp},
            device_id_type=pl.DeviceIdType.MESH,
        )

    def arrival(target, recv):
        return remote(target, target, weight_send.at[0], recv, d, m)

    def turn(index):
        low = 2 * spot < line
        above = line - 1 - spot
        first = jnp.where(low, above, spot)
        early = jnp.where(low, line - 1 - index, index)
        late = jnp.where(low, index - first, line - 1 - (index - first))
        return jnp.where(index < first, early, late)

    def quarter(index):
        return grad_ref.at[pl.ds(pl.multiple_of(index * part, part), part), :]

    weight_copy = remote(
        weight_ref, weight_all.at[:, own_columns], weight_send.at[0], weight_recv.at[0], twin, m
    )
    weight_here = pltpu.make_async_copy(
        weight_ref, weight_all.at[:, own_columns], weight_recv.at[1]
    )

    def direct(step, c):
        target = lax.rem(tier + step, tiers)
        index = c * tiers + target
        return remote(
            quarter(index),
            grads.at[spot, index],
            swap_send.at[step, c],
            grad_recv.at[spot, index],
            2 * m + side,
            2 * target + c,
        )

    def stay():
        return pltpu.make_async_copy(quarter(place), grads.at[spot, place], grad_recv.at[spot, place])

    def relay(step, c):
        target = lax.rem(tier + step, tiers)
        return remote(
            quarter(c * tiers + target),
            relay_in.at[step, c],
            swap_send.at[step, c],
            relay_recv.at[step, c],
            d,
            2 * target + core,
        )

    def relay_origin(step):
        return 2 * lax.rem(tier + tiers - step, tiers) + core

    def onward(step, c):
        return remote(
            relay_in.at[step, c],
            grads.at[spot, c * tiers + tier],
            relay_send.at[step, c],
            grad_recv.at[spot, c * tiers + tier],
            2 * relay_origin(step) + side,
            2 * tier + c,
        )

    def swaps(act, local):
        for step in range(1, tiers):
            for c in range(2):
                @pl.when(at_home)
                def _(step=step, c=c):
                    act(direct(step, c))

                @pl.when(jnp.logical_not(at_home))
                def _(step=step, c=c):
                    act(relay(step, c))

        for c in range(2):
            mine = at_home & (core == c)

            @pl.when(mine)
            def _():
                local()

            @pl.when(jnp.logical_not(mine))
            def _(c=c):
                act(direct(0, c))

    barrier = pltpu.get_barrier_semaphore()

    def greet(dp, mp):
        pl.semaphore_signal(
            barrier, inc=1, device_id={"dp": dp, "mp": mp}, device_id_type=pl.DeviceIdType.MESH
        )

    greet(twin, m)
    for step in reversed(range(line)):
        for other in range(n_mp):
            if step or other:
                greet(lax.rem(d + 2 * step, n_dp), lax.rem(m + other, n_mp))
    loads = [
        pltpu.make_async_copy(source, target, load_recv.at[index])
        for index, (source, target) in enumerate(
            (
                (lengths_hbm, lengths_ref),
                (query_hbm, query_ref),
                (key_hbm, key_ref),
                (value_hbm, value_ref),
            )
        )
    ]
    for copy in loads:
        copy.start()
    weight_here.start()
    for copy in loads:
        copy.wait()

    allowed = allowed_pairs(lengths_ref, rows)
    for h in range(head_count):
        kv = h // group_size
        head = slice(h * HEAD_WIDTH, (h + 1) * HEAD_WIDTH)
        kv_head = slice(kv * HEAD_WIDTH, (kv + 1) * HEAD_WIDTH)
        logits = dot(query_ref[:, head], key_ref[:, kv_head], NT) * scale
        logits = jnp.where(allowed, logits, -jnp.inf)
        exp_terms = jnp.exp(logits - jnp.max(logits, axis=1, keepdims=True))
        probability = exp_terms / jnp.sum(exp_terms, axis=1, keepdims=True)
        probs[h] = probability
        heads_all[spot, :, head] = dot(
            probability.astype(jnp.bfloat16), value_ref[:, kv_head], NN
        ).astype(jnp.bfloat16)

    pl.semaphore_wait(barrier, line * n_mp)
    swaps(lambda copy: copy.start(), lambda: stay().start())
    weight_copy.start()

    def heads_copy(block, way):
        return remote(
            heads_all.at[block],
            heads_all.at[block],
            heads_send.at[block, way],
            heads_recv.at[block],
            (d + 2, d - 2)[way],
            m,
        )

    def heads_pass(distance, started):
        for way, sign in ((0, -1), (1, 1)):
            block = spot + sign * distance
            target = spot - sign

            @pl.when((block >= 0) & (block < line))
            def _(block=block, way=way, target=target):
                if started and distance > 0:
                    arrival(heads_all.at[block], heads_recv.at[block]).wait_recv()

                @pl.when((target >= 0) & (target < line))
                def _():
                    if started:
                        heads_copy(block, way).start()
                    else:
                        heads_copy(block, way).wait_send()

    heads_pass(0, True)

    def lift(block, step):
        target = lax.rem(tier + step, tiers)
        return remote(
            grads.at[block, place],
            grads.at[block, place],
            lift_send.at[block, step],
            grad_recv.at[block, place],
            d,
            2 * target + core,
        )

    def near(distance, act):
        if distance == 0:
            act(spot)
        else:
            for sign in (-1, 1):
                block = spot + sign * distance

                @pl.when((block >= 0) & (block < line))
                def _(block=block):
                    act(block)

    def lift_begin(block):
        arrival(grads.at[block, place], grad_recv.at[block, place]).wait_recv()
        for step in range(1, tiers):
            lift(block, step).start()

    near(0, lift_begin)
    for step in range(1, tiers):
        for c in range(2):
            @pl.when(relay_origin(step) != spot)
            def _(step=step, c=c):
                arrival(relay_in.at[step, c], relay_recv.at[step, c]).wait_recv()
                onward(step, c).start()

    near(1, lift_begin)
    heads_pass(1, True)
    for distance in range(2, line):
        near(distance, lift_begin)

    def layer_begin(block):
        layer_part[block] = dot(heads_all[block], weight_all[...], NN).astype(jnp.bfloat16).reshape(
            n_mp, part, span
        )
        pair_copy(block).start()
        turned = heads_all[block].astype(jnp.float32).T.astype(jnp.bfloat16)
        heads_turned[block] = turned

    def pair_copy(block):
        return remote(
            layer_part.at[block, sibling_half],
            pair_in.at[block],
            pair_send.at[block],
            pair_recv.at[block],
            d,
            sibling,
        )

    def tier_copy(block, step):
        target = lax.rem(tier + step, tiers)
        return remote(
            pair_out.at[block, step],
            tier_in.at[block, step],
            tier_send.at[block, step],
            tier_recv.at[block, step],
            d,
            2 * target + core,
        )

    def layer_pair(block):
        arrival(pair_in.at[block], pair_recv.at[block]).wait_recv()
        for step in range(1, tiers):
            target = lax.rem(tier + step, tiers)
            pair_out[block, step] = (
                layer_part[block, core * tiers + target].astype(jnp.float32)
                + pair_in[block, target].astype(jnp.float32)
            ).astype(jnp.bfloat16)
            tier_copy(block, step).start()

    def done_copy(block):
        return remote(
            layer_sum.at[block],
            layer_in.at[place],
            done_send.at[block],
            done_recv.at[place],
            2 * block + side,
            spot,
        )

    def layer_end(block):
        total = layer_part[block, place].astype(jnp.float32) + pair_in[block, tier].astype(
            jnp.float32
        )
        for step in range(1, tiers):
            arrival(tier_in.at[block, step], tier_recv.at[block, step]).wait_recv()
            total = total + tier_in[block, step].astype(jnp.float32)
        total = total.astype(jnp.bfloat16)
        here = at_home & (block == spot)

        @pl.when(here)
        def _():
            layer_in[place] = total

        @pl.when(jnp.logical_not(here))
        def _():
            layer_sum[block] = total
            done_copy(block).start()

    def side_copy(block):
        return remote(
            grads.at[block, own_half],
            grads.at[block, own_half],
            side_send.at[block],
            side_recv.at[block],
            d,
            sibling,
        )

    def side_begin(block):
        for step in range(1, tiers):
            from_place = core * tiers + lax.rem(tier + step, tiers)
            arrival(grads.at[block, from_place], grad_recv.at[block, from_place]).wait_recv()
        side_copy(block).start()

    def up_copy(block, way):
        return remote(
            up_out.at[block],
            up_in.at[way, block],
            up_send.at[block],
            up_recv.at[way, block],
            (d + 2, d - 2)[way],
            m,
        )

    def up_block(block):
        arrival(grads.at[block, sibling_half], side_recv.at[block]).wait_recv()
        up_own[block] = dot(grads[block].reshape(rows, span), weight_all[...], NT)

    def up_pass(index, started):
        block = turn(index)
        for way, sign in ((0, 1), (1, -1)):
            origin = spot - sign

            @pl.when((block - spot) * sign > 0)
            def _(way=way, origin=origin):
                if started:
                    inner = (origin >= 0) & (origin < line)

                    @pl.when(inner)
                    def _():
                        arrival(up_in.at[way, block], up_recv.at[way, block]).wait_recv()
                        up_out[block] = (
                            up_own[block] + up_in[way, block].astype(jnp.float32)
                        ).astype(jnp.bfloat16)

                    @pl.when(jnp.logical_not(inner))
                    def _():
                        up_out[block] = up_own[block].astype(jnp.bfloat16)

                    up_copy(block, way).start()
                else:
                    up_copy(block, way).wait_send()

    twin_copy = remote(twin_out, twin_in, twin_send.at[0], twin_recv.at[0], twin, m)

    def weight_half(which):
        total = dot(heads_turned[0], grads[0, :, :, which].reshape(rows, columns), NN)
        for block in range(1, line):
            total = total + dot(
                heads_turned[block], grads[block, :, :, which].reshape(rows, columns), NN
            )
        return total

    arrival(weight_all.at[:, twin_columns], weight_recv.at[0]).wait_recv()
    weight_here.wait()
    layer_begin(spot)
    near(0, side_begin)
    near(1, side_begin)
    near(0, up_block)
    heads_pass(2, True)
    for distance in range(2, line):
        near(distance, side_begin)
        near(distance - 1, up_block)
    near(line - 1, up_block)
    edge = (spot == 0) | (spot == line - 1)

    def up_turn(index):
        @pl.when(jnp.logical_not(edge))
        def _():
            up_pass(index, True)

    def edge_step(index, carry):
        up_pass(index, True)
        return carry

    @pl.when(edge)
    def _():
        lax.fori_loop(0, line - 1, edge_step, 0)

    near(0, layer_pair)
    near(1, layer_begin)
    for distance in range(2, line - 1):
        near(distance - 1, layer_pair)
        near(distance, layer_begin)
        if distance > 2:
            heads_pass(distance, True)
    for index in range(line - 2):
        up_turn(index)
        if index == 0:
            heads_pass(line - 1, True)
            near(line - 2, layer_pair)
            near(line - 1, layer_begin)
    twin_out[...] = weight_half(twin_columns).astype(jnp.bfloat16)
    twin_copy.start()
    near(line - 1, layer_pair)
    near(0, layer_end)
    up_turn(line - 2)
    for distance in range(1, line):
        near(distance, layer_end)
    weight_grad_ref[...] = weight_half(own_columns)

    for way, sign in ((0, -1), (1, 1)):
        @pl.when((spot + sign >= 0) & (spot + sign < line))
        def _(way=way):
            arrival(up_in.at[way, spot], up_recv.at[way, spot]).wait_recv()
            up_own[spot] = up_own[spot] + up_in[way, spot].astype(jnp.float32)

    for h in range(head_count):
        kv = h // group_size
        head = slice(h * HEAD_WIDTH, (h + 1) * HEAD_WIDTH)
        kv_head = slice(kv * HEAD_WIDTH, (kv + 1) * HEAD_WIDTH)
        upstream = up_own[spot, :, head].astype(jnp.bfloat16)
        probability = probs[h]
        prob_grad = dot(upstream, value_ref[:, kv_head], NT)
        row_delta = jnp.sum(probability * prob_grad, axis=1, keepdims=True)
        score_grad = (probability * (prob_grad - row_delta) * scale).astype(jnp.bfloat16)
        query_grad_ref[:, head] = dot(score_grad, key_ref[:, kv_head], NN).astype(jnp.bfloat16)
        key_term = dot(score_grad, query_ref[:, head], TN)
        value_term = dot(probability.astype(jnp.bfloat16), upstream, TN)
        if h % group_size == 0:
            key_sum, value_sum = key_term, value_term
        else:
            key_sum, value_sum = key_sum + key_term, value_sum + value_term
        if h % group_size == group_size - 1:
            key_grad_ref[:, kv_head] = key_sum.astype(jnp.bfloat16)
            value_grad_ref[:, kv_head] = value_sum.astype(jnp.bfloat16)

    arrival(twin_in, twin_recv.at[0]).wait_recv()
    weight_grad_ref[...] += twin_in[...].astype(jnp.float32)

    for c in range(2):
        for level in range(tiers):
            @pl.when(jnp.logical_not(at_home & (place == c * tiers + level)))
            def _(index=c * tiers + level):
                arrival(layer_in.at[index], done_recv.at[index]).wait_recv()

    layer_ref[...] = layer_in[...].reshape(rows, span)

    swaps(lambda copy: copy.wait_send(), lambda: None)
    weight_copy.wait_send()
    for step in range(1, tiers):
        for c in range(2):
            @pl.when(relay_origin(step) != spot)
            def _(step=step, c=c):
                onward(step, c).wait_send()

    for distance in range(line - 1):
        heads_pass(distance, False)
    twin_copy.wait_send()

    def drain_step(block, carry):
        side_copy(block).wait_send()
        pair_copy(block).wait_send()
        for step in range(1, tiers):
            lift(block, step).wait_send()
            tier_copy(block, step).wait_send()

        @pl.when(jnp.logical_not(at_home & (block == spot)))
        def _():
            done_copy(block).wait_send()

        @pl.when(block < line - 1)
        def _():
            up_pass(block, False)

        return carry

    lax.fori_loop(0, line, drain_step, 0)


def finish_kernel(*refs):
    count = len(refs) // 2
    sems = refs[-1]
    copies = [
        pltpu.make_async_copy(refs[index], refs[count + index], sems.at[index])
        for index in range(count)
    ]
    for copy in copies:
        copy.start()
    for copy in copies:
        copy.wait()


def finish(arrays):
    anywhere = pl.BlockSpec(memory_space=pl.ANY)
    return pl.pallas_call(
        finish_kernel,
        out_shape=tuple(jax.ShapeDtypeStruct(a.shape, a.dtype) for a in arrays),
        in_specs=[anywhere] * len(arrays),
        out_specs=(pl.BlockSpec(memory_space=pltpu.HBM),) * len(arrays),
        scratch_shapes=[pltpu.SemaphoreType.DMA((len(arrays),))],
        compiler_params=pltpu.CompilerParams(vmem_limit_bytes=1024 * 1024),
    )(*arrays)


def fused(n_dp, n_mp, query_rows, key_rows, value_matrix, out_weight, out_grad, doc_lengths):
    rows, width = query_rows.shape
    columns = out_weight.shape[1]
    span = out_grad.shape[1]
    line = n_dp // 2
    tiers = n_mp // 2
    part = rows // n_mp
    vmem = pl.BlockSpec(memory_space=pltpu.VMEM)
    hbm = pl.BlockSpec(memory_space=pltpu.HBM)
    dma = pltpu.SemaphoreType.DMA
    bf16 = jnp.bfloat16
    return pl.pallas_call(
        functools.partial(branch_kernel, n_dp, n_mp),
        out_shape=(
            jax.ShapeDtypeStruct(out_grad.shape, bf16),
            jax.ShapeDtypeStruct(query_rows.shape, bf16),
            jax.ShapeDtypeStruct(key_rows.shape, bf16),
            jax.ShapeDtypeStruct(value_matrix.shape, bf16),
            jax.ShapeDtypeStruct(out_weight.shape, jnp.float32),
        ),
        in_specs=[hbm] * 6,
        out_specs=(vmem,) * 5,
        scratch_shapes=[
            pltpu.SMEM(doc_lengths.shape, jnp.int32),
            pltpu.VMEM(query_rows.shape, bf16),
            pltpu.VMEM(key_rows.shape, bf16),
            pltpu.VMEM(value_matrix.shape, bf16),
            pltpu.VMEM((width, span), bf16),
            pltpu.VMEM((line, n_mp, part, span), bf16),
            pltpu.VMEM((tiers, 2, part, span), bf16),
            pltpu.VMEM((line, rows, width), bf16),
            pltpu.VMEM((line, width, rows), bf16),
            pltpu.VMEM((line, rows, width), jnp.float32),
            pltpu.VMEM((2, line, rows, width), bf16),
            pltpu.VMEM((line, rows, width), bf16),
            pltpu.VMEM((line, n_mp, part, span), bf16),
            pltpu.VMEM((line, tiers, part, span), bf16),
            pltpu.VMEM((line, tiers, part, span), bf16),
            pltpu.VMEM((line, tiers, part, span), bf16),
            pltpu.VMEM((line, part, span), bf16),
            pltpu.VMEM((n_mp, part, span), bf16),
            pltpu.VMEM((width, columns), bf16),
            pltpu.VMEM((width, columns), bf16),
            pltpu.VMEM((width // HEAD_WIDTH, rows, rows), jnp.float32),
            dma((1,)),
            dma((2,)),
            dma((tiers, 2)),
            dma((tiers, 2)),
            dma((tiers, 2)),
            dma((line, n_mp)),
            dma((line, tiers)),
            dma((line,)),
            dma((line,)),
            dma((line, 2)),
            dma((line,)),
            dma((line,)),
            dma((2, line)),
            dma((line,)),
            dma((line,)),
            dma((line, tiers)),
            dma((line, tiers)),
            dma((line,)),
            dma((n_mp,)),
            dma((1,)),
            dma((1,)),
            dma((4,)),
        ],
        compiler_params=pltpu.CompilerParams(
            has_side_effects=True, collective_id=0, vmem_limit_bytes=36 * 1024 * 1024
        ),
    )(*(pltpu.with_memory_space_constraint(a, pltpu.HBM) for a in (doc_lengths, query_rows, key_rows, value_matrix, out_weight, out_grad)))


def body_of(n_dp, n_mp):
    def body(query_rows, key_rows, value_matrix, out_weight, out_grad, doc_lengths):
        arrays = (query_rows, key_rows, value_matrix, out_weight, out_grad, doc_lengths)
        columns = out_weight.shape[1]
        rows, width = query_rows.shape
        held = 2 * n_dp * rows * (4 * columns + 3 * width)
        if (
            columns % 128 == 0
            and rows % 128 == 0
            and rows % (16 * n_mp) == 0
            and n_dp == 2 * n_mp
            and n_mp % 2 == 0
            and n_mp > 2
            and 2 * columns == out_grad.shape[1]
            and held < 24 * 1024 * 1024
        ):
            return finish(fused(n_dp, n_mp, *arrays))
        return per_device(*arrays)

    return body


def solution(mesh):
    placed = (
        P("dp", "mp"),
        P("dp", "mp"),
        P("dp", "mp"),
        P("mp", "dp"),
        P("dp", "mp"),
        P("dp", None),
    )
    return jax.shard_map(
        body_of(mesh.shape["dp"], mesh.shape["mp"]),
        mesh=mesh,
        in_specs=placed,
        out_specs=(P("dp", "mp"), P("dp", "mp"), P("dp", "mp"), P("dp", "mp"), P("mp", "dp")),
        check_vma=False,
    )
```

```python
import functools

import jax
import jax.numpy as jnp
from jax import lax
from jax.experimental import pallas as pl
from jax.experimental.pallas import tpu as pltpu
from jax.sharding import PartitionSpec as P

HEAD_WIDTH = 128
TILE = 128


def local_segments(lengths, row_count):
    segment_ends = jnp.cumsum(lengths)
    positions = jnp.arange(row_count, dtype=jnp.int32)
    return jnp.sum((positions[:, None] >= segment_ends[None, :]).astype(jnp.int32), axis=1)


def to_heads(matrix):
    return matrix.reshape(matrix.shape[0], matrix.shape[1] // HEAD_WIDTH, HEAD_WIDTH).transpose(
        1, 0, 2
    )


def from_heads(tensor):
    return tensor.transpose(1, 0, 2).reshape(tensor.shape[1], tensor.shape[0] * tensor.shape[2])


def attend(queries, key_rows, value_matrix, upstreams, segment):
    head_count, row_count, head_size = queries.shape
    tile_rows = min(TILE, row_count)
    block_count = row_count // tile_rows
    softmax_scale = HEAD_WIDTH ** (-0.5)
    offsets = jnp.arange(tile_rows, dtype=jnp.int32)
    empty_rows = jnp.zeros((tile_rows, head_size), jnp.float32)
    key_sums = [empty_rows] * block_count
    value_sums = [empty_rows] * block_count
    attended_blocks = []
    grad_blocks = []
    for block_index in range(block_count):
        row_start = block_index * tile_rows
        query_tile = queries[:, row_start : row_start + tile_rows]
        upstream_tile = upstreams[:, row_start : row_start + tile_rows]
        query_segment = segment[row_start : row_start + tile_rows]
        active = [
            segment[(column_index + 1) * tile_rows - 1] >= query_segment[0]
            for column_index in range(block_index + 1)
        ]
        score_tiles = []
        for column_index in range(block_index + 1):
            column_start = column_index * tile_rows
            key_tile = key_rows[column_start : column_start + tile_rows]
            key_segment = segment[column_start : column_start + tile_rows]
            allowed = (query_segment[:, None] == key_segment[None, :]) & (
                (row_start + offsets)[:, None] >= (column_start + offsets)[None, :]
            )

            def score_tile(query_tile=query_tile, key_tile=key_tile, allowed=allowed):
                logits = (
                    jnp.einsum(
                        "hid,jd->hij", query_tile, key_tile, preferred_element_type=jnp.float32
                    )
                    * softmax_scale
                )
                return jnp.where(allowed[None], logits, -jnp.inf)

            def masked_tile():
                return jnp.full((head_count, tile_rows, tile_rows), -jnp.inf, jnp.float32)

            score_tiles.append(lax.cond(active[column_index], score_tile, masked_tile))
        logits = jnp.concatenate(score_tiles, axis=-1)
        row_max = jnp.max(logits, axis=-1, keepdims=True)
        exp_terms = jnp.exp(logits - row_max)
        probability = exp_terms / jnp.sum(exp_terms, axis=-1, keepdims=True)
        weights = probability.astype(jnp.bfloat16)
        attended = jnp.zeros((head_count, tile_rows, head_size), jnp.float32)
        grad_tiles = []
        for column_index in range(block_index + 1):
            column_start = column_index * tile_rows
            value_tile = value_matrix[column_start : column_start + tile_rows]
            weight_tile = weights[:, :, column_start : column_start + tile_rows]

            def forward_tile(
                weight_tile=weight_tile, value_tile=value_tile, upstream_tile=upstream_tile
            ):
                return (
                    jnp.einsum(
                        "hij,jd->hid", weight_tile, value_tile, preferred_element_type=jnp.float32
                    ),
                    jnp.einsum(
                        "hid,jd->hij", upstream_tile, value_tile, preferred_element_type=jnp.float32
                    ),
                )

            def empty_pair():
                return (
                    jnp.zeros((head_count, tile_rows, head_size), jnp.float32),
                    jnp.zeros((head_count, tile_rows, tile_rows), jnp.float32),
                )

            contribution, prob_grad_tile = lax.cond(active[column_index], forward_tile, empty_pair)
            attended = attended + contribution
            grad_tiles.append(prob_grad_tile)
        prob_grad = jnp.concatenate(grad_tiles, axis=-1)
        row_delta = jnp.sum(probability * prob_grad, axis=-1, keepdims=True)
        score_grad = (probability * (prob_grad - row_delta) * softmax_scale).astype(jnp.bfloat16)
        query_sum = jnp.zeros((head_count, tile_rows, head_size), jnp.float32)
        for column_index in range(block_index + 1):
            column_start = column_index * tile_rows
            key_tile = key_rows[column_start : column_start + tile_rows]
            score_piece = score_grad[:, :, column_start : column_start + tile_rows]
            weight_tile = weights[:, :, column_start : column_start + tile_rows]

            def backward_tile(
                score_piece=score_piece,
                key_tile=key_tile,
                weight_tile=weight_tile,
                query_tile=query_tile,
                upstream_tile=upstream_tile,
            ):
                return (
                    jnp.einsum(
                        "hij,jd->hid", score_piece, key_tile, preferred_element_type=jnp.float32
                    ),
                    jnp.einsum(
                        "hij,hid->jd", score_piece, query_tile, preferred_element_type=jnp.float32
                    ),
                    jnp.einsum(
                        "hij,hid->jd",
                        weight_tile,
                        upstream_tile,
                        preferred_element_type=jnp.float32,
                    ),
                )

            def empty_triple():
                return (
                    jnp.zeros((head_count, tile_rows, head_size), jnp.float32),
                    empty_rows,
                    empty_rows,
                )

            query_part, key_part, value_part = lax.cond(
                active[column_index], backward_tile, empty_triple
            )
            query_sum = query_sum + query_part
            key_sums[column_index] = key_sums[column_index] + key_part
            value_sums[column_index] = value_sums[column_index] + value_part
        attended_blocks.append(attended.astype(jnp.bfloat16))
        grad_blocks.append(query_sum.astype(jnp.bfloat16))
    return (
        jnp.concatenate(attended_blocks, axis=1),
        jnp.concatenate(grad_blocks, axis=1),
        jnp.concatenate(key_sums, axis=0),
        jnp.concatenate(value_sums, axis=0),
    )


def grad_term(grad_full, attended_heads):
    attended_flat = from_heads(attended_heads)
    return lax.dot_general(
        grad_full, attended_flat, (((0,), (0,)), ((), ())), preferred_element_type=jnp.float32
    )


def per_device(query_rows, key_rows, value_matrix, out_weight, out_grad, doc_lengths):
    row_count = query_rows.shape[0]
    weight_full = lax.all_gather(out_weight, "dp", axis=1, tiled=True)
    grad_full = lax.all_gather(out_grad, "mp", axis=1, tiled=True)
    attn_grad = lax.dot_general(
        grad_full, weight_full, (((1,), (1,)), ((), ())), preferred_element_type=jnp.float32
    ).astype(jnp.bfloat16)
    segment = local_segments(doc_lengths[0], row_count)
    queries = to_heads(query_rows)
    upstreams = to_heads(attn_grad)
    attended, query_grad, key_sum, value_sum = attend(
        queries, key_rows, value_matrix, upstreams, segment
    )
    key_grad = key_sum.astype(jnp.bfloat16)
    value_grad = value_sum.astype(jnp.bfloat16)
    weight_part = lax.psum_scatter(
        grad_term(grad_full, attended), "dp", scatter_dimension=0, tiled=True
    )
    attended_flat = from_heads(attended)
    query_grad = from_heads(query_grad)
    partial_sum = jnp.dot(attended_flat, weight_full, preferred_element_type=jnp.float32).astype(
        jnp.bfloat16
    )
    layer_out = lax.psum_scatter(
        lax.optimization_barrier(partial_sum).astype(jnp.float32).astype(jnp.bfloat16),
        "mp",
        scatter_dimension=1,
        tiled=True,
    )
    return (layer_out, query_grad, key_grad, value_grad, weight_part.T)


def dot(a, b, dims):
    return lax.dot_general(a, b, (dims, ((), ())), preferred_element_type=jnp.float32)


NN = ((1,), (0,))
NT = ((1,), (1,))
TN = ((0,), (0,))


def allowed_pairs(lengths_ref, rows):
    row_at = lax.broadcasted_iota(jnp.int32, (rows, 1), 0)
    column_at = lax.broadcasted_iota(jnp.int32, (1, rows), 1)
    row_segment = jnp.zeros((rows, 1), jnp.int32)
    column_segment = jnp.zeros((1, rows), jnp.int32)
    end = jnp.int32(0)
    for index in range(lengths_ref.shape[1]):
        end = end + lengths_ref[0, index]
        row_segment = row_segment + jnp.where(row_at >= end, 1, 0)
        column_segment = column_segment + jnp.where(column_at >= end, 1, 0)
    return (row_segment == column_segment) & (row_at >= column_at)


def branch_kernel(
    n_dp,
    n_mp,
    lengths_hbm,
    query_hbm,
    key_hbm,
    value_hbm,
    weight_ref,
    grad_ref,
    layer_ref,
    query_grad_ref,
    key_grad_ref,
    value_grad_ref,
    weight_grad_ref,
    lengths_ref,
    query_ref,
    key_ref,
    value_ref,
    weight_all,
    grads,
    relay_in,
    heads_all,
    heads_turned,
    up_own,
    up_in,
    up_out,
    layer_part,
    pair_in,
    pair_out,
    tier_in,
    layer_sum,
    layer_in,
    twin_out,
    twin_in,
    probs,
    weight_send,
    weight_recv,
    swap_send,
    relay_send,
    relay_recv,
    grad_recv,
    lift_send,
    side_send,
    side_recv,
    heads_send,
    heads_recv,
    up_send,
    up_recv,
    pair_send,
    pair_recv,
    tier_send,
    tier_recv,
    done_send,
    done_recv,
    twin_send,
    twin_recv,
    load_recv,
):
    d = lax.axis_index("dp")
    m = lax.axis_index("mp")
    line = n_dp // 2
    tiers = n_mp // 2
    rows = query_ref.shape[0]
    part = rows // n_mp
    width = query_ref.shape[1]
    columns = weight_ref.shape[1]
    span = grad_ref.shape[1]
    head_count = width // HEAD_WIDTH
    group_size = width // key_ref.shape[1]
    scale = HEAD_WIDTH ** (-0.5)
    spot = lax.div(d, 2)
    side = lax.rem(d, 2)
    twin = d + 1 - 2 * side
    core = lax.rem(m, 2)
    tier = lax.div(m, 2)
    sibling = m + 1 - 2 * core
    place = core * tiers + tier
    own_columns = pl.ds(pl.multiple_of(side * columns, 128), columns)
    twin_columns = pl.ds(pl.multiple_of((1 - side) * columns, 128), columns)
    own_half = pl.ds(core * tiers, tiers)
    sibling_half = pl.ds((1 - core) * tiers, tiers)
    at_home = spot == m

    def remote(source, target, send, recv, dp, mp):
        return pltpu.make_async_remote_copy(
            src_ref=source,
            dst_ref=target,
            send_sem=send,
            recv_sem=recv,
            device_id={"dp": dp, "mp": mp},
            device_id_type=pl.DeviceIdType.MESH,
        )

    def arrival(target, recv):
        return remote(target, target, weight_send.at[0], recv, d, m)

    def quarter(index):
        return grad_ref.at[pl.ds(pl.multiple_of(index * part, part), part), :]

    weight_copy = remote(
        weight_ref, weight_all.at[:, own_columns], weight_send.at[0], weight_recv.at[0], twin, m
    )
    weight_here = pltpu.make_async_copy(
        weight_ref, weight_all.at[:, own_columns], weight_recv.at[1]
    )

    def direct(step, c):
        target = lax.rem(tier + step, tiers)
        index = c * tiers + target
        return remote(
            quarter(index),
            grads.at[spot, index],
            swap_send.at[step, c],
            grad_recv.at[spot, index],
            2 * m + side,
            2 * target + c,
        )

    def stay():
        return pltpu.make_async_copy(quarter(place), grads.at[spot, place], grad_recv.at[spot, place])

    def relay(step, c):
        target = lax.rem(tier + step, tiers)
        return remote(
            quarter(c * tiers + target),
            relay_in.at[step, c],
            swap_send.at[step, c],
            relay_recv.at[step, c],
            d,
            2 * target + core,
        )

    def relay_origin(step):
        return 2 * lax.rem(tier + tiers - step, tiers) + core

    def onward(step, c):
        return remote(
            relay_in.at[step, c],
            grads.at[spot, c * tiers + tier],
            relay_send.at[step, c],
            grad_recv.at[spot, c * tiers + tier],
            2 * relay_origin(step) + side,
            2 * tier + c,
        )

    def swaps(act, local):
        for step in range(1, tiers):
            for c in range(2):
                @pl.when(at_home)
                def _(step=step, c=c):
                    act(direct(step, c))

                @pl.when(jnp.logical_not(at_home))
                def _(step=step, c=c):
                    act(relay(step, c))

        for c in range(2):
            mine = at_home & (core == c)

            @pl.when(mine)
            def _():
                local()

            @pl.when(jnp.logical_not(mine))
            def _(c=c):
                act(direct(0, c))

    barrier = pltpu.get_barrier_semaphore()

    def greet(dp, mp):
        pl.semaphore_signal(
            barrier, inc=1, device_id={"dp": dp, "mp": mp}, device_id_type=pl.DeviceIdType.MESH
        )

    greet(twin, m)
    for step in reversed(range(line)):
        for other in range(n_mp):
            if step or other:
                greet(lax.rem(d + 2 * step, n_dp), lax.rem(m + other, n_mp))
    loads = [
        pltpu.make_async_copy(source, target, load_recv.at[index])
        for index, (source, target) in enumerate(
            (
                (lengths_hbm, lengths_ref),
                (query_hbm, query_ref),
                (key_hbm, key_ref),
                (value_hbm, value_ref),
            )
        )
    ]
    for copy in loads:
        copy.start()
    weight_here.start()
    for copy in loads:
        copy.wait()

    allowed = allowed_pairs(lengths_ref, rows)
    for h in range(head_count):
        kv = h // group_size
        head = slice(h * HEAD_WIDTH, (h + 1) * HEAD_WIDTH)
        kv_head = slice(kv * HEAD_WIDTH, (kv + 1) * HEAD_WIDTH)
        logits = dot(query_ref[:, head], key_ref[:, kv_head], NT) * scale
        logits = jnp.where(allowed, logits, -jnp.inf)
        exp_terms = jnp.exp(logits - jnp.max(logits, axis=1, keepdims=True))
        probability = exp_terms / jnp.sum(exp_terms, axis=1, keepdims=True)
        probs[h] = probability
        heads_all[spot, :, head] = dot(
            probability.astype(jnp.bfloat16), value_ref[:, kv_head], NN
        ).astype(jnp.bfloat16)

    pl.semaphore_wait(barrier, line * n_mp)
    swaps(lambda copy: copy.start(), lambda: stay().start())
    weight_copy.start()

    def heads_copy(block, way):
        return remote(
            heads_all.at[block],
            heads_all.at[block],
            heads_send.at[block, way],
            heads_recv.at[block],
            (d + 2, d - 2)[way],
            m,
        )

    def heads_pass(distance, started):
        for way, sign in ((0, -1), (1, 1)):
            block = spot + sign * distance
            target = spot - sign

            @pl.when((block >= 0) & (block < line))
            def _(block=block, way=way, target=target):
                if started and distance > 0:
                    arrival(heads_all.at[block], heads_recv.at[block]).wait_recv()

                @pl.when((target >= 0) & (target < line))
                def _():
                    if started:
                        heads_copy(block, way).start()
                    else:
                        heads_copy(block, way).wait_send()

    heads_pass(0, True)

    def lift(block, step):
        target = lax.rem(tier + step, tiers)
        return remote(
            grads.at[block, place],
            grads.at[block, place],
            lift_send.at[block, step],
            grad_recv.at[block, place],
            d,
            2 * target + core,
        )

    def near(distance, act):
        if distance == 0:
            act(spot)
        else:
            for sign in (-1, 1):
                block = spot + sign * distance

                @pl.when((block >= 0) & (block < line))
                def _(block=block):
                    act(block)

    def lift_begin(block):
        arrival(grads.at[block, place], grad_recv.at[block, place]).wait_recv()
        for step in range(1, tiers):
            lift(block, step).start()

    near(0, lift_begin)
    for step in range(1, tiers):
        for c in range(2):
            @pl.when(relay_origin(step) != spot)
            def _(step=step, c=c):
                arrival(relay_in.at[step, c], relay_recv.at[step, c]).wait_recv()
                onward(step, c).start()

    near(1, lift_begin)
    heads_pass(1, True)
    for distance in range(2, line):
        near(distance, lift_begin)

    def layer_begin(block):
        layer_part[block] = dot(heads_all[block], weight_all[...], NN).astype(jnp.bfloat16).reshape(
            n_mp, part, span
        )
        pair_copy(block).start()
        turned = heads_all[block].astype(jnp.float32).T.astype(jnp.bfloat16)
        heads_turned[block] = turned

    def pair_copy(block):
        return remote(
            layer_part.at[block, sibling_half],
            pair_in.at[block],
            pair_send.at[block],
            pair_recv.at[block],
            d,
            sibling,
        )

    def tier_copy(block, step):
        target = lax.rem(tier + step, tiers)
        return remote(
            pair_out.at[block, step],
            tier_in.at[block, step],
            tier_send.at[block, step],
            tier_recv.at[block, step],
            d,
            2 * target + core,
        )

    def layer_pair(block):
        arrival(pair_in.at[block], pair_recv.at[block]).wait_recv()
        for step in range(1, tiers):
            target = lax.rem(tier + step, tiers)
            pair_out[block, step] = (
                layer_part[block, core * tiers + target].astype(jnp.float32)
                + pair_in[block, target].astype(jnp.float32)
            ).astype(jnp.bfloat16)
            tier_copy(block, step).start()

    def done_copy(block):
        return remote(
            layer_sum.at[block],
            layer_in.at[place],
            done_send.at[block],
            done_recv.at[place],
            2 * block + side,
            spot,
        )

    def layer_end(block):
        total = layer_part[block, place].astype(jnp.float32) + pair_in[block, tier].astype(
            jnp.float32
        )
        for step in range(1, tiers):
            arrival(tier_in.at[block, step], tier_recv.at[block, step]).wait_recv()
            total = total + tier_in[block, step].astype(jnp.float32)
        total = total.astype(jnp.bfloat16)
        here = at_home & (block == spot)

        @pl.when(here)
        def _():
            layer_in[place] = total

        @pl.when(jnp.logical_not(here))
        def _():
            layer_sum[block] = total
            done_copy(block).start()

    def side_copy(block):
        return remote(
            grads.at[block, own_half],
            grads.at[block, own_half],
            side_send.at[block],
            side_recv.at[block],
            d,
            sibling,
        )

    def side_begin(block):
        for step in range(1, tiers):
            from_place = core * tiers + lax.rem(tier + step, tiers)
            arrival(grads.at[block, from_place], grad_recv.at[block, from_place]).wait_recv()
        side_copy(block).start()

    middle = line // 2
    low = spot < middle
    gate = jnp.where(low, middle - 1, middle)
    far_gate = jnp.where(low, middle, middle - 1)
    edge = (spot == 0) | (spot == line - 1)

    def up_final(block):
        return remote(
            up_out.at[block],
            up_in.at[1, spot],
            up_send.at[block],
            up_recv.at[1, spot],
            2 * block + side,
            m,
        )

    def up_chain(block):
        return remote(
            up_out.at[block],
            up_in.at[0, block],
            up_send.at[block],
            up_recv.at[0, block],
            jnp.where(low, d + 2, d - 2),
            m,
        )

    def up_block(block):
        arrival(grads.at[block, sibling_half], side_recv.at[block]).wait_recv()
        up_own[block] = dot(grads[block].reshape(rows, span), weight_all[...], NT)
        crosses = ((block < middle) != low) & (block != far_gate)

        @pl.when(jnp.logical_not(crosses) & (block != spot))
        def _():
            up_out[block] = up_own[block].astype(jnp.bfloat16)
            up_final(block).start()

        @pl.when(crosses & edge)
        def _():
            up_out[block] = up_own[block].astype(jnp.bfloat16)
            up_chain(block).start()

    def up_gather(index):
        block = jnp.where(low, middle + index, middle - 1 - index)

        @pl.when(jnp.logical_not(edge))
        def _():
            arrival(up_in.at[0, block], up_recv.at[0, block]).wait_recv()
            up_out[block] = (up_own[block] + up_in[0, block].astype(jnp.float32)).astype(
                jnp.bfloat16
            )

            @pl.when(spot == gate)
            def _():
                up_final(block).start()

            @pl.when(spot != gate)
            def _():
                up_chain(block).start()

    twin_copy = remote(twin_out, twin_in, twin_send.at[0], twin_recv.at[0], twin, m)

    def weight_half(which):
        total = dot(heads_turned[0], grads[0, :, :, which].reshape(rows, columns), NN)
        for block in range(1, line):
            total = total + dot(
                heads_turned[block], grads[block, :, :, which].reshape(rows, columns), NN
            )
        return total

    arrival(weight_all.at[:, twin_columns], weight_recv.at[0]).wait_recv()
    weight_here.wait()
    layer_begin(spot)
    near(0, side_begin)
    layer_pair(spot)
    near(1, layer_begin)
    near(1, side_begin)
    near(0, up_block)
    near(1, layer_pair)
    for distance in range(2, line - 1):
        heads_pass(distance, True)
        near(distance, side_begin)
        near(distance - 1, up_block)
    near(line - 2, up_block)
    near(line - 1, side_begin)
    near(line - 1, up_block)
    for distance in range(2, line):
        if distance == line - 1:
            heads_pass(distance, True)
        if distance > 2:
            near(distance - 1, layer_pair)
        near(distance, layer_begin)
    near(line - 1, layer_pair)
    layer_end(spot)
    twin_out[...] = weight_half(twin_columns).astype(jnp.bfloat16)
    twin_copy.start()
    near(1, layer_end)
    for index in range(1, middle):
        up_gather(index)
        near(index + 1, layer_end)
    for distance in range(middle + 1, line):
        near(distance, layer_end)
    weight_grad_ref[...] = weight_half(own_columns)

    def up_add(source):
        arrival(up_in.at[1, source], up_recv.at[1, source]).wait_recv()
        up_own[spot] = up_own[spot] + up_in[1, source].astype(jnp.float32)

    for index in range(middle):
        source = jnp.where(low, index, middle + index)

        @pl.when(source != spot)
        def _(source=source):
            up_add(source)

    up_add(far_gate)
    for index in range(middle):
        source = jnp.where(low, middle + index, index)

        @pl.when((spot == gate) & (source != far_gate))
        def _(source=source):
            up_add(source)

    for h in range(head_count):
        kv = h // group_size
        head = slice(h * HEAD_WIDTH, (h + 1) * HEAD_WIDTH)
        kv_head = slice(kv * HEAD_WIDTH, (kv + 1) * HEAD_WIDTH)
        upstream = up_own[spot, :, head].astype(jnp.bfloat16)
        probability = probs[h]
        prob_grad = dot(upstream, value_ref[:, kv_head], NT)
        row_delta = jnp.sum(probability * prob_grad, axis=1, keepdims=True)
        score_grad = (probability * (prob_grad - row_delta) * scale).astype(jnp.bfloat16)
        query_grad_ref[:, head] = dot(score_grad, key_ref[:, kv_head], NN).astype(jnp.bfloat16)
        key_term = dot(score_grad, query_ref[:, head], TN)
        value_term = dot(probability.astype(jnp.bfloat16), upstream, TN)
        if h % group_size == 0:
            key_sum, value_sum = key_term, value_term
        else:
            key_sum, value_sum = key_sum + key_term, value_sum + value_term
        if h % group_size == group_size - 1:
            key_grad_ref[:, kv_head] = key_sum.astype(jnp.bfloat16)
            value_grad_ref[:, kv_head] = value_sum.astype(jnp.bfloat16)

    arrival(twin_in, twin_recv.at[0]).wait_recv()
    weight_grad_ref[...] += twin_in[...].astype(jnp.float32)

    for c in range(2):
        for level in range(tiers):
            @pl.when(jnp.logical_not(at_home & (place == c * tiers + level)))
            def _(index=c * tiers + level):
                arrival(layer_in.at[index], done_recv.at[index]).wait_recv()

    layer_ref[...] = layer_in[...].reshape(rows, span)

    swaps(lambda copy: copy.wait_send(), lambda: None)
    weight_copy.wait_send()
    for step in range(1, tiers):
        for c in range(2):
            @pl.when(relay_origin(step) != spot)
            def _(step=step, c=c):
                onward(step, c).wait_send()

    for distance in range(line - 1):
        heads_pass(distance, False)
    twin_copy.wait_send()

    def drain_step(block, carry):
        side_copy(block).wait_send()
        pair_copy(block).wait_send()
        for step in range(1, tiers):
            lift(block, step).wait_send()
            tier_copy(block, step).wait_send()

        @pl.when(jnp.logical_not(at_home & (block == spot)))
        def _():
            done_copy(block).wait_send()

        @pl.when(block != spot)
        def _():
            up_final(block).wait_send()

        return carry

    lax.fori_loop(0, line, drain_step, 0)


def finish_kernel(*refs):
    count = len(refs) // 2
    sems = refs[-1]
    copies = [
        pltpu.make_async_copy(refs[index], refs[count + index], sems.at[index])
        for index in range(count)
    ]
    for copy in copies:
        copy.start()
    for copy in copies:
        copy.wait()


def finish(arrays):
    anywhere = pl.BlockSpec(memory_space=pl.ANY)
    return pl.pallas_call(
        finish_kernel,
        out_shape=tuple(jax.ShapeDtypeStruct(a.shape, a.dtype) for a in arrays),
        in_specs=[anywhere] * len(arrays),
        out_specs=(pl.BlockSpec(memory_space=pltpu.HBM),) * len(arrays),
        scratch_shapes=[pltpu.SemaphoreType.DMA((len(arrays),))],
        compiler_params=pltpu.CompilerParams(vmem_limit_bytes=1024 * 1024),
    )(*arrays)


def fused(n_dp, n_mp, query_rows, key_rows, value_matrix, out_weight, out_grad, doc_lengths):
    rows, width = query_rows.shape
    columns = out_weight.shape[1]
    span = out_grad.shape[1]
    line = n_dp // 2
    tiers = n_mp // 2
    part = rows // n_mp
    vmem = pl.BlockSpec(memory_space=pltpu.VMEM)
    hbm = pl.BlockSpec(memory_space=pltpu.HBM)
    dma = pltpu.SemaphoreType.DMA
    bf16 = jnp.bfloat16
    return pl.pallas_call(
        functools.partial(branch_kernel, n_dp, n_mp),
        out_shape=(
            jax.ShapeDtypeStruct(out_grad.shape, bf16),
            jax.ShapeDtypeStruct(query_rows.shape, bf16),
            jax.ShapeDtypeStruct(key_rows.shape, bf16),
            jax.ShapeDtypeStruct(value_matrix.shape, bf16),
            jax.ShapeDtypeStruct(out_weight.shape, jnp.float32),
        ),
        in_specs=[hbm] * 6,
        out_specs=(vmem,) * 5,
        scratch_shapes=[
            pltpu.SMEM(doc_lengths.shape, jnp.int32),
            pltpu.VMEM(query_rows.shape, bf16),
            pltpu.VMEM(key_rows.shape, bf16),
            pltpu.VMEM(value_matrix.shape, bf16),
            pltpu.VMEM((width, span), bf16),
            pltpu.VMEM((line, n_mp, part, span), bf16),
            pltpu.VMEM((tiers, 2, part, span), bf16),
            pltpu.VMEM((line, rows, width), bf16),
            pltpu.VMEM((line, width, rows), bf16),
            pltpu.VMEM((line, rows, width), jnp.float32),
            pltpu.VMEM((2, line, rows, width), bf16),
            pltpu.VMEM((line, rows, width), bf16),
            pltpu.VMEM((line, n_mp, part, span), bf16),
            pltpu.VMEM((line, tiers, part, span), bf16),
            pltpu.VMEM((line, tiers, part, span), bf16),
            pltpu.VMEM((line, tiers, part, span), bf16),
            pltpu.VMEM((line, part, span), bf16),
            pltpu.VMEM((n_mp, part, span), bf16),
            pltpu.VMEM((width, columns), bf16),
            pltpu.VMEM((width, columns), bf16),
            pltpu.VMEM((width // HEAD_WIDTH, rows, rows), jnp.float32),
            dma((1,)),
            dma((2,)),
            dma((tiers, 2)),
            dma((tiers, 2)),
            dma((tiers, 2)),
            dma((line, n_mp)),
            dma((line, tiers)),
            dma((line,)),
            dma((line,)),
            dma((line, 2)),
            dma((line,)),
            dma((line,)),
            dma((2, line)),
            dma((line,)),
            dma((line,)),
            dma((line, tiers)),
            dma((line, tiers)),
            dma((line,)),
            dma((n_mp,)),
            dma((1,)),
            dma((1,)),
            dma((4,)),
        ],
        compiler_params=pltpu.CompilerParams(
            has_side_effects=True, collective_id=0, vmem_limit_bytes=36 * 1024 * 1024
        ),
    )(*(pltpu.with_memory_space_constraint(a, pltpu.HBM) for a in (doc_lengths, query_rows, key_rows, value_matrix, out_weight, out_grad)))


def body_of(n_dp, n_mp):
    def body(query_rows, key_rows, value_matrix, out_weight, out_grad, doc_lengths):
        arrays = (query_rows, key_rows, value_matrix, out_weight, out_grad, doc_lengths)
        columns = out_weight.shape[1]
        rows, width = query_rows.shape
        held = 2 * n_dp * rows * (4 * columns + 3 * width)
        if (
            columns % 128 == 0
            and rows % 128 == 0
            and rows % (16 * n_mp) == 0
            and n_dp == 2 * n_mp
            and n_mp % 2 == 0
            and n_mp > 2
            and 2 * columns == out_grad.shape[1]
            and held < 24 * 1024 * 1024
        ):
            return finish(fused(n_dp, n_mp, *arrays))
        return per_device(*arrays)

    return body


def solution(mesh):
    placed = (
        P("dp", "mp"),
        P("dp", "mp"),
        P("dp", "mp"),
        P("mp", "dp"),
        P("dp", "mp"),
        P("dp", None),
    )
    return jax.shard_map(
        body_of(mesh.shape["dp"], mesh.shape["mp"]),
        mesh=mesh,
        in_specs=placed,
        out_specs=(P("dp", "mp"), P("dp", "mp"), P("dp", "mp"), P("dp", "mp"), P("mp", "dp")),
        check_vma=False,
    )
```

```python
import functools

import jax
import jax.numpy as jnp
from jax import lax
from jax.experimental import pallas as pl
from jax.experimental.pallas import tpu as pltpu
from jax.sharding import PartitionSpec as P

HEAD_WIDTH = 128
TILE = 128


def local_segments(lengths, row_count):
    segment_ends = jnp.cumsum(lengths)
    positions = jnp.arange(row_count, dtype=jnp.int32)
    return jnp.sum((positions[:, None] >= segment_ends[None, :]).astype(jnp.int32), axis=1)


def to_heads(matrix):
    return matrix.reshape(matrix.shape[0], matrix.shape[1] // HEAD_WIDTH, HEAD_WIDTH).transpose(
        1, 0, 2
    )


def from_heads(tensor):
    return tensor.transpose(1, 0, 2).reshape(tensor.shape[1], tensor.shape[0] * tensor.shape[2])


def attend(queries, key_rows, value_matrix, upstreams, segment):
    head_count, row_count, head_size = queries.shape
    tile_rows = min(TILE, row_count)
    block_count = row_count // tile_rows
    softmax_scale = HEAD_WIDTH ** (-0.5)
    offsets = jnp.arange(tile_rows, dtype=jnp.int32)
    empty_rows = jnp.zeros((tile_rows, head_size), jnp.float32)
    key_sums = [empty_rows] * block_count
    value_sums = [empty_rows] * block_count
    attended_blocks = []
    grad_blocks = []
    for block_index in range(block_count):
        row_start = block_index * tile_rows
        query_tile = queries[:, row_start : row_start + tile_rows]
        upstream_tile = upstreams[:, row_start : row_start + tile_rows]
        query_segment = segment[row_start : row_start + tile_rows]
        active = [
            segment[(column_index + 1) * tile_rows - 1] >= query_segment[0]
            for column_index in range(block_index + 1)
        ]
        score_tiles = []
        for column_index in range(block_index + 1):
            column_start = column_index * tile_rows
            key_tile = key_rows[column_start : column_start + tile_rows]
            key_segment = segment[column_start : column_start + tile_rows]
            allowed = (query_segment[:, None] == key_segment[None, :]) & (
                (row_start + offsets)[:, None] >= (column_start + offsets)[None, :]
            )

            def score_tile(query_tile=query_tile, key_tile=key_tile, allowed=allowed):
                logits = (
                    jnp.einsum(
                        "hid,jd->hij", query_tile, key_tile, preferred_element_type=jnp.float32
                    )
                    * softmax_scale
                )
                return jnp.where(allowed[None], logits, -jnp.inf)

            def masked_tile():
                return jnp.full((head_count, tile_rows, tile_rows), -jnp.inf, jnp.float32)

            score_tiles.append(lax.cond(active[column_index], score_tile, masked_tile))
        logits = jnp.concatenate(score_tiles, axis=-1)
        row_max = jnp.max(logits, axis=-1, keepdims=True)
        exp_terms = jnp.exp(logits - row_max)
        probability = exp_terms / jnp.sum(exp_terms, axis=-1, keepdims=True)
        weights = probability.astype(jnp.bfloat16)
        attended = jnp.zeros((head_count, tile_rows, head_size), jnp.float32)
        grad_tiles = []
        for column_index in range(block_index + 1):
            column_start = column_index * tile_rows
            value_tile = value_matrix[column_start : column_start + tile_rows]
            weight_tile = weights[:, :, column_start : column_start + tile_rows]

            def forward_tile(
                weight_tile=weight_tile, value_tile=value_tile, upstream_tile=upstream_tile
            ):
                return (
                    jnp.einsum(
                        "hij,jd->hid", weight_tile, value_tile, preferred_element_type=jnp.float32
                    ),
                    jnp.einsum(
                        "hid,jd->hij", upstream_tile, value_tile, preferred_element_type=jnp.float32
                    ),
                )

            def empty_pair():
                return (
                    jnp.zeros((head_count, tile_rows, head_size), jnp.float32),
                    jnp.zeros((head_count, tile_rows, tile_rows), jnp.float32),
                )

            contribution, prob_grad_tile = lax.cond(active[column_index], forward_tile, empty_pair)
            attended = attended + contribution
            grad_tiles.append(prob_grad_tile)
        prob_grad = jnp.concatenate(grad_tiles, axis=-1)
        row_delta = jnp.sum(probability * prob_grad, axis=-1, keepdims=True)
        score_grad = (probability * (prob_grad - row_delta) * softmax_scale).astype(jnp.bfloat16)
        query_sum = jnp.zeros((head_count, tile_rows, head_size), jnp.float32)
        for column_index in range(block_index + 1):
            column_start = column_index * tile_rows
            key_tile = key_rows[column_start : column_start + tile_rows]
            score_piece = score_grad[:, :, column_start : column_start + tile_rows]
            weight_tile = weights[:, :, column_start : column_start + tile_rows]

            def backward_tile(
                score_piece=score_piece,
                key_tile=key_tile,
                weight_tile=weight_tile,
                query_tile=query_tile,
                upstream_tile=upstream_tile,
            ):
                return (
                    jnp.einsum(
                        "hij,jd->hid", score_piece, key_tile, preferred_element_type=jnp.float32
                    ),
                    jnp.einsum(
                        "hij,hid->jd", score_piece, query_tile, preferred_element_type=jnp.float32
                    ),
                    jnp.einsum(
                        "hij,hid->jd",
                        weight_tile,
                        upstream_tile,
                        preferred_element_type=jnp.float32,
                    ),
                )

            def empty_triple():
                return (
                    jnp.zeros((head_count, tile_rows, head_size), jnp.float32),
                    empty_rows,
                    empty_rows,
                )

            query_part, key_part, value_part = lax.cond(
                active[column_index], backward_tile, empty_triple
            )
            query_sum = query_sum + query_part
            key_sums[column_index] = key_sums[column_index] + key_part
            value_sums[column_index] = value_sums[column_index] + value_part
        attended_blocks.append(attended.astype(jnp.bfloat16))
        grad_blocks.append(query_sum.astype(jnp.bfloat16))
    return (
        jnp.concatenate(attended_blocks, axis=1),
        jnp.concatenate(grad_blocks, axis=1),
        jnp.concatenate(key_sums, axis=0),
        jnp.concatenate(value_sums, axis=0),
    )


def grad_term(grad_full, attended_heads):
    attended_flat = from_heads(attended_heads)
    return lax.dot_general(
        grad_full, attended_flat, (((0,), (0,)), ((), ())), preferred_element_type=jnp.float32
    )


def per_device(query_rows, key_rows, value_matrix, out_weight, out_grad, doc_lengths):
    row_count = query_rows.shape[0]
    weight_full = lax.all_gather(out_weight, "dp", axis=1, tiled=True)
    grad_full = lax.all_gather(out_grad, "mp", axis=1, tiled=True)
    attn_grad = lax.dot_general(
        grad_full, weight_full, (((1,), (1,)), ((), ())), preferred_element_type=jnp.float32
    ).astype(jnp.bfloat16)
    segment = local_segments(doc_lengths[0], row_count)
    queries = to_heads(query_rows)
    upstreams = to_heads(attn_grad)
    attended, query_grad, key_sum, value_sum = attend(
        queries, key_rows, value_matrix, upstreams, segment
    )
    key_grad = key_sum.astype(jnp.bfloat16)
    value_grad = value_sum.astype(jnp.bfloat16)
    weight_part = lax.psum_scatter(
        grad_term(grad_full, attended), "dp", scatter_dimension=0, tiled=True
    )
    attended_flat = from_heads(attended)
    query_grad = from_heads(query_grad)
    partial_sum = jnp.dot(attended_flat, weight_full, preferred_element_type=jnp.float32).astype(
        jnp.bfloat16
    )
    layer_out = lax.psum_scatter(
        lax.optimization_barrier(partial_sum).astype(jnp.float32).astype(jnp.bfloat16),
        "mp",
        scatter_dimension=1,
        tiled=True,
    )
    return (layer_out, query_grad, key_grad, value_grad, weight_part.T)


def dot(a, b, dims):
    return lax.dot_general(a, b, (dims, ((), ())), preferred_element_type=jnp.float32)


NN = ((1,), (0,))
NT = ((1,), (1,))
TN = ((0,), (0,))


def allowed_pairs(lengths_ref, rows):
    row_at = lax.broadcasted_iota(jnp.int32, (rows, 1), 0)
    column_at = lax.broadcasted_iota(jnp.int32, (1, rows), 1)
    row_segment = jnp.zeros((rows, 1), jnp.int32)
    column_segment = jnp.zeros((1, rows), jnp.int32)
    end = jnp.int32(0)
    for index in range(lengths_ref.shape[1]):
        end = end + lengths_ref[0, index]
        row_segment = row_segment + jnp.where(row_at >= end, 1, 0)
        column_segment = column_segment + jnp.where(column_at >= end, 1, 0)
    return (row_segment == column_segment) & (row_at >= column_at)


def branch_kernel(
    n_dp,
    n_mp,
    lengths_hbm,
    query_hbm,
    key_hbm,
    value_hbm,
    weight_ref,
    grad_ref,
    layer_ref,
    query_grad_ref,
    key_grad_ref,
    value_grad_ref,
    weight_grad_ref,
    lengths_ref,
    query_ref,
    key_ref,
    value_ref,
    weight_all,
    grads,
    relay_in,
    heads_all,
    heads_turned,
    up_own,
    up_in,
    up_out,
    layer_part,
    pair_in,
    pair_out,
    tier_in,
    layer_sum,
    layer_in,
    twin_out,
    twin_in,
    probs,
    weight_send,
    weight_recv,
    swap_send,
    relay_send,
    relay_recv,
    grad_recv,
    lift_send,
    side_send,
    side_recv,
    heads_send,
    heads_recv,
    up_send,
    up_recv,
    pair_send,
    pair_recv,
    tier_send,
    tier_recv,
    done_send,
    done_recv,
    twin_send,
    twin_recv,
    load_recv,
):
    d = lax.axis_index("dp")
    m = lax.axis_index("mp")
    line = n_dp // 2
    tiers = n_mp // 2
    rows = query_ref.shape[0]
    part = rows // n_mp
    width = query_ref.shape[1]
    columns = weight_ref.shape[1]
    span = grad_ref.shape[1]
    head_count = width // HEAD_WIDTH
    group_size = width // key_ref.shape[1]
    scale = HEAD_WIDTH ** (-0.5)
    spot = lax.div(d, 2)
    side = lax.rem(d, 2)
    twin = d + 1 - 2 * side
    core = lax.rem(m, 2)
    tier = lax.div(m, 2)
    sibling = m + 1 - 2 * core
    place = core * tiers + tier
    own_columns = pl.ds(pl.multiple_of(side * columns, 128), columns)
    twin_columns = pl.ds(pl.multiple_of((1 - side) * columns, 128), columns)
    own_half = pl.ds(core * tiers, tiers)
    sibling_half = pl.ds((1 - core) * tiers, tiers)
    at_home = spot == m

    def remote(source, target, send, recv, dp, mp):
        return pltpu.make_async_remote_copy(
            src_ref=source,
            dst_ref=target,
            send_sem=send,
            recv_sem=recv,
            device_id={"dp": dp, "mp": mp},
            device_id_type=pl.DeviceIdType.MESH,
        )

    def arrival(target, recv):
        return remote(target, target, weight_send.at[0], recv, d, m)

    def quarter(index):
        return grad_ref.at[pl.ds(pl.multiple_of(index * part, part), part), :]

    weight_copy = remote(
        weight_ref, weight_all.at[:, own_columns], weight_send.at[0], weight_recv.at[0], twin, m
    )
    weight_here = pltpu.make_async_copy(
        weight_ref, weight_all.at[:, own_columns], weight_recv.at[1]
    )

    def direct(step, c):
        target = lax.rem(tier + step, tiers)
        index = c * tiers + target
        return remote(
            quarter(index),
            grads.at[spot, index],
            swap_send.at[step, c],
            grad_recv.at[spot, index],
            2 * m + side,
            2 * target + c,
        )

    def stay():
        return pltpu.make_async_copy(quarter(place), grads.at[spot, place], grad_recv.at[spot, place])

    def relay(step, c):
        target = lax.rem(tier + step, tiers)
        return remote(
            quarter(c * tiers + target),
            relay_in.at[step, c],
            swap_send.at[step, c],
            relay_recv.at[step, c],
            d,
            2 * target + core,
        )

    def relay_origin(step):
        return 2 * lax.rem(tier + tiers - step, tiers) + core

    def onward(step, c):
        return remote(
            relay_in.at[step, c],
            grads.at[spot, c * tiers + tier],
            relay_send.at[step, c],
            grad_recv.at[spot, c * tiers + tier],
            2 * relay_origin(step) + side,
            2 * tier + c,
        )

    def swaps(act, local):
        for step in range(1, tiers):
            for c in range(2):
                @pl.when(at_home)
                def _(step=step, c=c):
                    act(direct(step, c))

                @pl.when(jnp.logical_not(at_home))
                def _(step=step, c=c):
                    act(relay(step, c))

        for c in range(2):
            mine = at_home & (core == c)

            @pl.when(mine)
            def _():
                local()

            @pl.when(jnp.logical_not(mine))
            def _(c=c):
                act(direct(0, c))

    barrier = pltpu.get_barrier_semaphore()

    def greet(dp, mp):
        pl.semaphore_signal(
            barrier, inc=1, device_id={"dp": dp, "mp": mp}, device_id_type=pl.DeviceIdType.MESH
        )

    greet(twin, m)
    for step in reversed(range(line)):
        for other in range(n_mp):
            if step or other:
                greet(lax.rem(d + 2 * step, n_dp), lax.rem(m + other, n_mp))
    loads = [
        pltpu.make_async_copy(source, target, load_recv.at[index])
        for index, (source, target) in enumerate(
            (
                (lengths_hbm, lengths_ref),
                (query_hbm, query_ref),
                (key_hbm, key_ref),
                (value_hbm, value_ref),
            )
        )
    ]
    for copy in loads:
        copy.start()
    weight_here.start()
    for copy in loads:
        copy.wait()

    allowed = allowed_pairs(lengths_ref, rows)
    for h in range(head_count):
        kv = h // group_size
        head = slice(h * HEAD_WIDTH, (h + 1) * HEAD_WIDTH)
        kv_head = slice(kv * HEAD_WIDTH, (kv + 1) * HEAD_WIDTH)
        logits = dot(query_ref[:, head], key_ref[:, kv_head], NT) * scale
        logits = jnp.where(allowed, logits, -jnp.inf)
        exp_terms = jnp.exp(logits - jnp.max(logits, axis=1, keepdims=True))
        probability = exp_terms / jnp.sum(exp_terms, axis=1, keepdims=True)
        probs[h] = probability
        heads_all[spot, :, head] = dot(
            probability.astype(jnp.bfloat16), value_ref[:, kv_head], NN
        ).astype(jnp.bfloat16)

    pl.semaphore_wait(barrier, line * n_mp)
    swaps(lambda copy: copy.start(), lambda: stay().start())
    weight_copy.start()

    def heads_copy(block, way):
        return remote(
            heads_all.at[block],
            heads_all.at[block],
            heads_send.at[block, way],
            heads_recv.at[block],
            (d + 2, d - 2)[way],
            m,
        )

    def heads_pass(distance, started):
        for way, sign in ((0, -1), (1, 1)):
            block = spot + sign * distance
            target = spot - sign

            @pl.when((block >= 0) & (block < line))
            def _(block=block, way=way, target=target):
                if started and distance > 0:
                    arrival(heads_all.at[block], heads_recv.at[block]).wait_recv()

                @pl.when((target >= 0) & (target < line))
                def _():
                    if started:
                        heads_copy(block, way).start()
                    else:
                        heads_copy(block, way).wait_send()

    heads_pass(0, True)

    def lift(block, step):
        target = lax.rem(tier + step, tiers)
        return remote(
            grads.at[block, place],
            grads.at[block, place],
            lift_send.at[block, step],
            grad_recv.at[block, place],
            d,
            2 * target + core,
        )

    def near(distance, act):
        if distance == 0:
            act(spot)
        else:
            for sign in (-1, 1):
                block = spot + sign * distance

                @pl.when((block >= 0) & (block < line))
                def _(block=block):
                    act(block)

    def lift_begin(block):
        arrival(grads.at[block, place], grad_recv.at[block, place]).wait_recv()
        for step in range(1, tiers):
            lift(block, step).start()

    near(0, lift_begin)
    for step in range(1, tiers):
        for c in range(2):
            @pl.when(relay_origin(step) != spot)
            def _(step=step, c=c):
                arrival(relay_in.at[step, c], relay_recv.at[step, c]).wait_recv()
                onward(step, c).start()

    near(1, lift_begin)
    heads_pass(1, True)
    for distance in range(2, line):
        near(distance, lift_begin)

    def layer_begin(block):
        layer_part[block] = dot(heads_all[block], weight_all[...], NN).astype(jnp.bfloat16).reshape(
            n_mp, part, span
        )
        pair_copy(block).start()
        turned = heads_all[block].astype(jnp.float32).T.astype(jnp.bfloat16)
        heads_turned[block] = turned

    def pair_copy(block):
        return remote(
            layer_part.at[block, sibling_half],
            pair_in.at[block],
            pair_send.at[block],
            pair_recv.at[block],
            d,
            sibling,
        )

    def tier_copy(block, step):
        target = lax.rem(tier + step, tiers)
        return remote(
            pair_out.at[block, step],
            tier_in.at[block, step],
            tier_send.at[block, step],
            tier_recv.at[block, step],
            d,
            2 * target + core,
        )

    def layer_pair(block):
        arrival(pair_in.at[block], pair_recv.at[block]).wait_recv()
        for step in range(1, tiers):
            target = lax.rem(tier + step, tiers)
            pair_out[block, step] = (
                layer_part[block, core * tiers + target].astype(jnp.float32)
                + pair_in[block, target].astype(jnp.float32)
            ).astype(jnp.bfloat16)
            tier_copy(block, step).start()

    def done_copy(block):
        return remote(
            layer_sum.at[block],
            layer_in.at[place],
            done_send.at[block],
            done_recv.at[place],
            2 * block + side,
            spot,
        )

    def layer_end(block):
        total = layer_part[block, place].astype(jnp.float32) + pair_in[block, tier].astype(
            jnp.float32
        )
        for step in range(1, tiers):
            arrival(tier_in.at[block, step], tier_recv.at[block, step]).wait_recv()
            total = total + tier_in[block, step].astype(jnp.float32)
        total = total.astype(jnp.bfloat16)
        here = at_home & (block == spot)

        @pl.when(here)
        def _():
            layer_in[place] = total

        @pl.when(jnp.logical_not(here))
        def _():
            layer_sum[block] = total
            done_copy(block).start()

    def side_copy(block):
        return remote(
            grads.at[block, own_half],
            grads.at[block, own_half],
            side_send.at[block],
            side_recv.at[block],
            d,
            sibling,
        )

    def side_begin(block):
        for step in range(1, tiers):
            from_place = core * tiers + lax.rem(tier + step, tiers)
            arrival(grads.at[block, from_place], grad_recv.at[block, from_place]).wait_recv()
        side_copy(block).start()

    middle = line // 2
    low = spot < middle
    gate = jnp.where(low, middle - 1, middle)
    far_gate = jnp.where(low, middle, middle - 1)
    edge = (spot == 0) | (spot == line - 1)

    def up_final(block):
        return remote(
            up_out.at[block],
            up_in.at[1, spot],
            up_send.at[block],
            up_recv.at[1, spot],
            2 * block + side,
            m,
        )

    def up_chain(block):
        return remote(
            up_out.at[block],
            up_in.at[0, block],
            up_send.at[block],
            up_recv.at[0, block],
            jnp.where(low, d + 2, d - 2),
            m,
        )

    def up_block(block):
        arrival(grads.at[block, sibling_half], side_recv.at[block]).wait_recv()
        up_own[block] = dot(grads[block].reshape(rows, span), weight_all[...], NT)
        crosses = ((block < middle) != low) & (block != far_gate)

        @pl.when(jnp.logical_not(crosses) & (block != spot))
        def _():
            up_out[block] = up_own[block].astype(jnp.bfloat16)
            up_final(block).start()

        @pl.when(crosses & edge)
        def _():
            up_out[block] = up_own[block].astype(jnp.bfloat16)
            up_chain(block).start()

    def up_gather(index):
        block = jnp.where(low, middle + index, middle - 1 - index)

        @pl.when(jnp.logical_not(edge))
        def _():
            arrival(up_in.at[0, block], up_recv.at[0, block]).wait_recv()
            up_out[block] = (up_own[block] + up_in[0, block].astype(jnp.float32)).astype(
                jnp.bfloat16
            )

            @pl.when(spot == gate)
            def _():
                up_final(block).start()

            @pl.when(spot != gate)
            def _():
                up_chain(block).start()

    twin_copy = remote(twin_out, twin_in, twin_send.at[0], twin_recv.at[0], twin, m)

    def weight_half(which):
        total = dot(heads_turned[0], grads[0, :, :, which].reshape(rows, columns), NN)
        for block in range(1, line):
            total = total + dot(
                heads_turned[block], grads[block, :, :, which].reshape(rows, columns), NN
            )
        return total

    arrival(weight_all.at[:, twin_columns], weight_recv.at[0]).wait_recv()
    weight_here.wait()
    layer_begin(spot)
    near(0, side_begin)
    layer_pair(spot)
    near(1, layer_begin)
    near(1, side_begin)
    near(1, layer_pair)
    near(1, up_block)
    near(0, up_block)
    for distance in range(2, line - 1):
        heads_pass(distance, True)
        near(distance, side_begin)
        near(distance, up_block)
    near(line - 1, side_begin)
    near(line - 1, up_block)
    for distance in range(2, line):
        if distance == line - 1:
            heads_pass(distance, True)
        if distance > 2:
            near(distance - 1, layer_pair)
        near(distance, layer_begin)
    near(line - 1, layer_pair)
    layer_end(spot)
    twin_out[...] = weight_half(twin_columns).astype(jnp.bfloat16)
    twin_copy.start()
    near(1, layer_end)
    for index in range(1, middle):
        up_gather(index)
        near(index + 1, layer_end)
    for distance in range(middle + 1, line):
        near(distance, layer_end)
    weight_grad_ref[...] = weight_half(own_columns)

    def up_add(source):
        arrival(up_in.at[1, source], up_recv.at[1, source]).wait_recv()
        up_own[spot] = up_own[spot] + up_in[1, source].astype(jnp.float32)

    for index in range(middle):
        source = jnp.where(low, index, middle + index)

        @pl.when(source != spot)
        def _(source=source):
            up_add(source)

    up_add(far_gate)
    for index in range(middle):
        source = jnp.where(low, middle + index, index)

        @pl.when((spot == gate) & (source != far_gate))
        def _(source=source):
            up_add(source)

    for h in range(head_count):
        kv = h // group_size
        head = slice(h * HEAD_WIDTH, (h + 1) * HEAD_WIDTH)
        kv_head = slice(kv * HEAD_WIDTH, (kv + 1) * HEAD_WIDTH)
        upstream = up_own[spot, :, head].astype(jnp.bfloat16)
        probability = probs[h]
        prob_grad = dot(upstream, value_ref[:, kv_head], NT)
        row_delta = jnp.sum(probability * prob_grad, axis=1, keepdims=True)
        score_grad = (probability * (prob_grad - row_delta) * scale).astype(jnp.bfloat16)
        query_grad_ref[:, head] = dot(score_grad, key_ref[:, kv_head], NN).astype(jnp.bfloat16)
        key_term = dot(score_grad, query_ref[:, head], TN)
        value_term = dot(probability.astype(jnp.bfloat16), upstream, TN)
        if h % group_size == 0:
            key_sum, value_sum = key_term, value_term
        else:
            key_sum, value_sum = key_sum + key_term, value_sum + value_term
        if h % group_size == group_size - 1:
            key_grad_ref[:, kv_head] = key_sum.astype(jnp.bfloat16)
            value_grad_ref[:, kv_head] = value_sum.astype(jnp.bfloat16)

    arrival(twin_in, twin_recv.at[0]).wait_recv()
    weight_grad_ref[...] += twin_in[...].astype(jnp.float32)

    for c in range(2):
        for level in range(tiers):
            @pl.when(jnp.logical_not(at_home & (place == c * tiers + level)))
            def _(index=c * tiers + level):
                arrival(layer_in.at[index], done_recv.at[index]).wait_recv()

    layer_ref[...] = layer_in[...].reshape(rows, span)

    swaps(lambda copy: copy.wait_send(), lambda: None)
    weight_copy.wait_send()
    for step in range(1, tiers):
        for c in range(2):
            @pl.when(relay_origin(step) != spot)
            def _(step=step, c=c):
                onward(step, c).wait_send()

    for distance in range(line - 1):
        heads_pass(distance, False)
    twin_copy.wait_send()

    def drain_step(block, carry):
        side_copy(block).wait_send()
        pair_copy(block).wait_send()
        for step in range(1, tiers):
            lift(block, step).wait_send()
            tier_copy(block, step).wait_send()

        @pl.when(jnp.logical_not(at_home & (block == spot)))
        def _():
            done_copy(block).wait_send()

        @pl.when(block != spot)
        def _():
            up_final(block).wait_send()

        return carry

    lax.fori_loop(0, line, drain_step, 0)


def finish_kernel(*refs):
    count = len(refs) // 2
    sems = refs[-1]
    copies = [
        pltpu.make_async_copy(refs[index], refs[count + index], sems.at[index])
        for index in range(count)
    ]
    for copy in copies:
        copy.start()
    for copy in copies:
        copy.wait()


def finish(arrays):
    anywhere = pl.BlockSpec(memory_space=pl.ANY)
    return pl.pallas_call(
        finish_kernel,
        out_shape=tuple(jax.ShapeDtypeStruct(a.shape, a.dtype) for a in arrays),
        in_specs=[anywhere] * len(arrays),
        out_specs=(pl.BlockSpec(memory_space=pltpu.HBM),) * len(arrays),
        scratch_shapes=[pltpu.SemaphoreType.DMA((len(arrays),))],
        compiler_params=pltpu.CompilerParams(vmem_limit_bytes=1024 * 1024),
    )(*arrays)


def fused(n_dp, n_mp, query_rows, key_rows, value_matrix, out_weight, out_grad, doc_lengths):
    rows, width = query_rows.shape
    columns = out_weight.shape[1]
    span = out_grad.shape[1]
    line = n_dp // 2
    tiers = n_mp // 2
    part = rows // n_mp
    vmem = pl.BlockSpec(memory_space=pltpu.VMEM)
    hbm = pl.BlockSpec(memory_space=pltpu.HBM)
    dma = pltpu.SemaphoreType.DMA
    bf16 = jnp.bfloat16
    return pl.pallas_call(
        functools.partial(branch_kernel, n_dp, n_mp),
        out_shape=(
            jax.ShapeDtypeStruct(out_grad.shape, bf16),
            jax.ShapeDtypeStruct(query_rows.shape, bf16),
            jax.ShapeDtypeStruct(key_rows.shape, bf16),
            jax.ShapeDtypeStruct(value_matrix.shape, bf16),
            jax.ShapeDtypeStruct(out_weight.shape, jnp.float32),
        ),
        in_specs=[hbm] * 6,
        out_specs=(vmem,) * 5,
        scratch_shapes=[
            pltpu.SMEM(doc_lengths.shape, jnp.int32),
            pltpu.VMEM(query_rows.shape, bf16),
            pltpu.VMEM(key_rows.shape, bf16),
            pltpu.VMEM(value_matrix.shape, bf16),
            pltpu.VMEM((width, span), bf16),
            pltpu.VMEM((line, n_mp, part, span), bf16),
            pltpu.VMEM((tiers, 2, part, span), bf16),
            pltpu.VMEM((line, rows, width), bf16),
            pltpu.VMEM((line, width, rows), bf16),
            pltpu.VMEM((line, rows, width), jnp.float32),
            pltpu.VMEM((2, line, rows, width), bf16),
            pltpu.VMEM((line, rows, width), bf16),
            pltpu.VMEM((line, n_mp, part, span), bf16),
            pltpu.VMEM((line, tiers, part, span), bf16),
            pltpu.VMEM((line, tiers, part, span), bf16),
            pltpu.VMEM((line, tiers, part, span), bf16),
            pltpu.VMEM((line, part, span), bf16),
            pltpu.VMEM((n_mp, part, span), bf16),
            pltpu.VMEM((width, columns), bf16),
            pltpu.VMEM((width, columns), bf16),
            pltpu.VMEM((width // HEAD_WIDTH, rows, rows), jnp.float32),
            dma((1,)),
            dma((2,)),
            dma((tiers, 2)),
            dma((tiers, 2)),
            dma((tiers, 2)),
            dma((line, n_mp)),
            dma((line, tiers)),
            dma((line,)),
            dma((line,)),
            dma((line, 2)),
            dma((line,)),
            dma((line,)),
            dma((2, line)),
            dma((line,)),
            dma((line,)),
            dma((line, tiers)),
            dma((line, tiers)),
            dma((line,)),
            dma((n_mp,)),
            dma((1,)),
            dma((1,)),
            dma((4,)),
        ],
        compiler_params=pltpu.CompilerParams(
            has_side_effects=True, collective_id=0, vmem_limit_bytes=36 * 1024 * 1024
        ),
    )(*(pltpu.with_memory_space_constraint(a, pltpu.HBM) for a in (doc_lengths, query_rows, key_rows, value_matrix, out_weight, out_grad)))


def body_of(n_dp, n_mp):
    def body(query_rows, key_rows, value_matrix, out_weight, out_grad, doc_lengths):
        arrays = (query_rows, key_rows, value_matrix, out_weight, out_grad, doc_lengths)
        columns = out_weight.shape[1]
        rows, width = query_rows.shape
        held = 2 * n_dp * rows * (4 * columns + 3 * width)
        if (
            columns % 128 == 0
            and rows % 128 == 0
            and rows % (16 * n_mp) == 0
            and n_dp == 2 * n_mp
            and n_mp % 2 == 0
            and n_mp > 2
            and 2 * columns == out_grad.shape[1]
            and held < 24 * 1024 * 1024
        ):
            return finish(fused(n_dp, n_mp, *arrays))
        return per_device(*arrays)

    return body


def solution(mesh):
    placed = (
        P("dp", "mp"),
        P("dp", "mp"),
        P("dp", "mp"),
        P("mp", "dp"),
        P("dp", "mp"),
        P("dp", None),
    )
    return jax.shard_map(
        body_of(mesh.shape["dp"], mesh.shape["mp"]),
        mesh=mesh,
        in_specs=placed,
        out_specs=(P("dp", "mp"), P("dp", "mp"), P("dp", "mp"), P("dp", "mp"), P("mp", "dp")),
        check_vma=False,
    )
```
